32 devices in a mesh: dp: 8 (over z, x), expert: 4 (over y, core).
Axes of the slice: x: 2, y: 2, z: 4, core: 2. Of those that a mesh axis runs over, the one named last changes fastest.
Arguments:
- tokens: bfloat16 [4096, 2048], P(('dp', 'expert')), may hold values from -6 to 6
- out_grad: bfloat16 [4096, 2048], P(('dp', 'expert')), may hold values from -3 to 3
- z_weight: float32 [4096], P(('dp', 'expert')), may hold values from 0.1 to 1
- router_weight: bfloat16 [2048, 128], replicated, may hold values from -0.125 to 0.125
- expert_ids: int32 [4096, 4], P(('dp', 'expert')), may hold values from 0 to 127, as said below
- gate_up_weight: bfloat16 [4, 2048, 3072], P('expert'), may hold values from -0.125 to 0.125
- down_weight: bfloat16 [4, 1536, 2048], P('expert'), may hold values from -0.15625 to 0.15625
Outputs:
- token_grad: bfloat16 [4096, 2048], P(('dp', 'expert'))
- router_grad: float32 [2048, 128], replicated
- gate_up_grad: bfloat16 [4, 2048, 3072], P('expert', 'dp')
- down_grad: bfloat16 [4, 1536, 2048], P('expert', 'dp')
The draws below stay inside these ranges and needn't reach their ends.
Inputs may be any that keep to these rules, and one draw needn't show every extreme that they name: `expert_ids`: each row names 4 different experts. Experts 0 to 3 are the ones in flight. The 128 rows of one device name any one expert in flight at most 64 times; in every data group some expert in flight is named exactly 64 times by the rows of each device of the group.
All inputs are finite; a program needn't handle non-finite values.
Results may differ from the reference program's by a relative error of at most 0.019.
Values may be sent and summed in bfloat16 or wider, within the bound.
A program may use at most 192 MiB of HBM per device.

```python
import math
import jax
import jax.numpy as jnp
from jax import lax

D = 2048
FF = 1536
ROUTED = 128
TOP = 4
BLOCK = 128
TOK_DEV = 128
CAP = 64
FLIGHT = 4
TOKENS = 4096
N_DP = 8
N_EXPERT = 4


def draw_expert_ids(key, part):
    devices_all = TOKENS // TOK_DEV
    flight = N_EXPERT
    key_base, key_mask, key_hot, key_dev = jax.random.split(key, 4)
    base = jax.random.randint(key_base, (devices_all, flight), 0, CAP + 1)
    base = base * jax.random.randint(key_mask, (devices_all, flight), 0, 2)
    hot = jax.random.randint(key_hot, (devices_all // N_EXPERT,), 0, flight)
    hot_dev = jnp.repeat(hot, N_EXPERT)
    counts = jnp.where(jnp.arange(flight)[None, :] == hot_dev[:, None], CAP, base).astype(jnp.int32)
    others = ROUTED - flight
    spacing = others // TOP

    def one_device(count_row, dev_key):
        key_fill, key_order, key_perm = jax.random.split(dev_key, 3)
        ends = jnp.cumsum(count_row)
        total = ends[-1]
        demand = jnp.arange(TOP * TOK_DEV, dtype=jnp.int32)
        owner = jnp.sum((ends[None, :] <= demand[:, None]).astype(jnp.int32), axis=1)
        table = jnp.where(demand < total, owner, -1).reshape(TOP, TOK_DEV).T
        offset = jax.random.randint(key_fill, (TOK_DEV, 1), 0, others)
        fill = flight + (offset + jnp.arange(TOP, dtype=jnp.int32)[None, :] * spacing) % others
        table = jnp.where(table >= 0, table, fill)
        order_keys = jax.random.randint(key_order, (TOK_DEV, TOP), 0, 1 << 20) * TOP + jnp.arange(TOP, dtype=jnp.int32)[None, :]
        order = jnp.argsort(order_keys, axis=1, stable=True)
        table = jnp.take_along_axis(table, order, axis=1)
        shuffle = jax.random.permutation(key_perm, TOK_DEV)
        return table[shuffle]
    dev_keys = jax.random.split(key_dev, devices_all)
    result = jax.vmap(one_device)(counts, dev_keys)
    return result.reshape(TOKENS, TOP).astype(jnp.int32)


def block_levels(rng, dims, cuts, smallest, high):
    level = 1.0
    for position, shards_of in cuts:
        heights = jax.random.uniform(jax.random.fold_in(jax.random.fold_in(rng, 6), position), (shards_of,), jnp.float32, smallest / len(cuts), high / len(cuts))
        level = level * jnp.repeat(jnp.exp(heights), dims[position] // shards_of).reshape((-1,) + (1,) * (len(dims) - 1 - position))
    return level


def normal_values(rng, extent, scale, limit, shards=(), kind=jnp.bfloat16):
    entries = scale * jax.random.normal(rng, extent, jnp.float32)
    if shards:
        entries = entries * block_levels(rng, extent, shards, -0.22, 0.18)
    return jnp.clip(entries, -limit, limit).astype(kind)


def setup_inputs(seed: int = 0) -> dict:
    key_list = jax.random.split(jax.random.key(seed), 8)
    tokens = normal_values(key_list[0], (TOKENS, D), 1.0, 6.0, ((0, 32),))
    out_grad = normal_values(key_list[1], (TOKENS, D), 0.5, 3.0, ((0, 32),))
    z_weight = jnp.clip(jnp.exp(math.log(1.0) - 2.3025851 * jax.random.uniform(key_list[2], (TOKENS,), jnp.float32) ** block_levels(key_list[2], (TOKENS,), ((0, 32),), -0.2, 0.2)), 0.1, 1.0)
    router_weight = normal_values(key_list[3], (D, ROUTED), D ** -0.5, 0.125)
    expert_ids = draw_expert_ids(jax.random.fold_in(key_list[7], 71), 0)
    gate_up_weight = normal_values(key_list[5], (FLIGHT, D, 2 * FF), D ** -0.5, 0.125, ((0, 4),))
    down_weight = normal_values(key_list[6], (FLIGHT, FF, D), FF ** -0.5, 0.15625, ((0, 4),))
    return dict(tokens=tokens, out_grad=out_grad, z_weight=z_weight, router_weight=router_weight, expert_ids=expert_ids, gate_up_weight=gate_up_weight, down_weight=down_weight)


def expert_rows(rows_in, rows_grad, w_gateup, w_down, acc_gateup, acc_down):
    hidden_units = w_down.shape[0]
    pre_act = jnp.dot(rows_in, w_gateup, preferred_element_type=jnp.float32)
    gate_pre = pre_act[:, :hidden_units]
    up_pre = pre_act[:, hidden_units:]
    activated = jax.nn.silu(gate_pre)
    hidden = (activated * up_pre).astype(jnp.bfloat16)
    expert_out = jnp.dot(hidden, w_down, preferred_element_type=jnp.float32).astype(jnp.bfloat16)
    hidden_grad = lax.dot_general(rows_grad, w_down, (((1,), (1,)), ((), ())), preferred_element_type=jnp.float32)
    acc_down = acc_down + lax.dot_general(hidden, rows_grad, (((0,), (0,)), ((), ())), preferred_element_type=jnp.float32)
    sigmoid_gate = jax.nn.sigmoid(gate_pre)
    gate_grad = hidden_grad * up_pre * sigmoid_gate * (1.0 + gate_pre * (1.0 - sigmoid_gate))
    up_grad = hidden_grad * activated
    pre_grad = jnp.concatenate([gate_grad, up_grad], axis=1).astype(jnp.bfloat16)
    acc_gateup = acc_gateup + lax.dot_general(rows_in, pre_grad, (((0,), (0,)), ((), ())), preferred_element_type=jnp.float32)
    input_grad = lax.dot_general(pre_grad, w_gateup, (((1,), (1,)), ((), ())), preferred_element_type=jnp.float32).astype(jnp.bfloat16)
    return acc_gateup, acc_down, expert_out, input_grad


def run_blocks(work_in, work_grad, w_gateup, w_down, nblocks):
    width = work_in.shape[1]
    hidden_units = w_down.shape[0]
    start_state = (jnp.zeros((width, 2 * hidden_units), jnp.float32), jnp.zeros((hidden_units, width), jnp.float32),
                   jnp.zeros_like(work_in), jnp.zeros_like(work_in))

    def step(block_index, carry):
        acc_gateup, acc_down, out_rows, grad_rows = carry
        start = (block_index * BLOCK).astype(jnp.int32)
        rows_in = lax.dynamic_slice_in_dim(work_in, start, BLOCK, 0)
        rows_grad = lax.dynamic_slice_in_dim(work_grad, start, BLOCK, 0)
        acc_gateup, acc_down, produced, backward = expert_rows(rows_in, rows_grad, w_gateup, w_down, acc_gateup, acc_down)
        out_rows = lax.dynamic_update_slice_in_dim(out_rows, produced, start, 0)
        grad_rows = lax.dynamic_update_slice_in_dim(grad_rows, backward, start, 0)
        return acc_gateup, acc_down, out_rows, grad_rows

    return lax.fori_loop(jnp.int32(0), nblocks.astype(jnp.int32), step, start_state)


def reference(tokens, out_grad, z_weight, router_weight, expert_ids, gate_up_weight, down_weight):
    logits = jnp.dot(tokens, router_weight, preferred_element_type=jnp.float32)
    choose = expert_ids[:, :, None] == jnp.arange(ROUTED, dtype=jnp.int32)[None, None, :]
    selected = jnp.sum(jnp.where(choose, logits[:, None, :], 0.0), axis=2)
    sel_exp = jnp.exp(selected)
    probs = sel_exp / jnp.sum(sel_exp, axis=1, keepdims=True)
    log_total = jnp.log(jnp.sum(jnp.exp(logits), axis=1))
    slots_group = N_EXPERT * TOK_DEV * TOP
    rows_max = N_EXPERT * CAP
    group_ids = expert_ids.reshape(N_DP, slots_group)
    group_prob = probs.reshape(N_DP, slots_group)
    group_tok = tokens.reshape(N_DP, N_EXPERT * TOK_DEV, D)
    group_grad = out_grad.reshape(N_DP, N_EXPERT * TOK_DEV, D)

    def one_group(carry, data):
        ids_here, prob_here, tok_here, grad_here = data

        def one_expert(expert):
            member = ids_here == expert
            rank = jnp.cumsum(member.astype(jnp.int32)) - 1
            place = jnp.where(member, rank, rows_max).astype(jnp.int32)
            source = jnp.zeros((rows_max,), jnp.int32).at[place].set(jnp.arange(slots_group, dtype=jnp.int32), mode="drop")
            valid = jnp.zeros((rows_max,), jnp.bool_).at[place].set(True, mode="drop")
            tok_index = source // TOP
            rows_in = jnp.where(valid[:, None], tok_here[tok_index], 0)
            rows_grad = jnp.where(valid[:, None], prob_here[source][:, None] * grad_here[tok_index].astype(jnp.float32), 0.0).astype(jnp.bfloat16)
            used = (jnp.sum(member.astype(jnp.int32)) + BLOCK - 1) // BLOCK
            acc_gateup, acc_down, produced, backward = run_blocks(rows_in, rows_grad, gate_up_weight[expert], down_weight[expert], used)
            return acc_gateup.astype(jnp.bfloat16), acc_down.astype(jnp.bfloat16), produced, backward, source, valid

        part_gu, part_down, outs, backs, sources, valids = lax.map(one_expert, jnp.arange(N_EXPERT, dtype=jnp.int32))
        sum_gu, sum_down = carry
        sum_gu = sum_gu + part_gu.astype(jnp.float32)
        sum_down = sum_down + part_down.astype(jnp.float32)
        target = jnp.where(valids.reshape(-1), sources.reshape(-1), slots_group).astype(jnp.int32)
        slot_out = jnp.zeros((slots_group, D), jnp.bfloat16).at[target].set(outs.reshape(-1, D), mode="drop")
        slot_back = jnp.zeros((slots_group, D), jnp.bfloat16).at[target].set(backs.reshape(-1, D), mode="drop")
        return (sum_gu, sum_down), (slot_out, slot_back)

    start_sums = (jnp.zeros((N_EXPERT, D, 2 * FF), jnp.float32), jnp.zeros((N_EXPERT, FF, D), jnp.float32))
    (sum_gu, sum_down), (slot_out, slot_back) = lax.scan(one_group, start_sums, (group_ids, group_prob, group_tok, group_grad))
    slot_out = slot_out.reshape(TOKENS, TOP, D)
    slot_back = slot_back.reshape(TOKENS, TOP, D)
    scores = jnp.sum(out_grad[:, None, :].astype(jnp.float32) * slot_out.astype(jnp.float32), axis=2)
    mean_score = jnp.sum(probs * scores, axis=1, keepdims=True)
    sel_grad = probs * (scores - mean_score)
    z_grad = 2.0 * z_weight[:, None] * log_total[:, None] * jnp.exp(logits - log_total[:, None])
    logit_grad = (z_grad + jnp.sum(jnp.where(choose, sel_grad[:, :, None], 0.0), axis=1)).astype(jnp.bfloat16)
    token_grad = (jnp.sum(slot_back.astype(jnp.float32), axis=1)
                  + lax.dot_general(logit_grad, router_weight, (((1,), (1,)), ((), ())), preferred_element_type=jnp.float32)).astype(jnp.bfloat16)
    router_grad = lax.dot_general(tokens, logit_grad, (((0,), (0,)), ((), ())), preferred_element_type=jnp.float32)
    return token_grad, router_grad, sum_gu.astype(jnp.bfloat16), sum_down.astype(jnp.bfloat16)
```

```python
import functools
import heapq
import itertools
import math

import jax
import jax.numpy as jnp
from jax import lax
from jax.experimental import pallas as pl
from jax.experimental.pallas import tpu as pltpu
from jax.sharding import PartitionSpec as P

F32 = jnp.float32
BF16 = jnp.bfloat16
MESH = pl.DeviceIdType.MESH
TOKENS, COTANGENTS, META, LOGIT = range(4)
LINK_RATE = 46.6e3
LINK_DELAY = 3.0


def lookup(table, key):
    value = jnp.int32(0)
    for slot, entry in enumerate(table):
        if entry:
            value = value + jnp.where(key == slot, jnp.int32(entry), jnp.int32(0))
    return value


def grid_of(copies, flight):
    inner = max(k for k in range(1, copies + 1) if copies % k == 0 and k * k <= copies)
    return dict(z=copies // inner, x=inner, y=flight // 2)


def visit_order(size):
    return [
        [i] + sorted((k for k in range(size) if k != i), key=lambda k: (abs(k - i), k < i))
        for i in range(size)
    ]


def make_parts(grid, tok_count):
    straight, crossed = ("x", "z", "y"), ("y", "z", "x")
    first_x, first_y = ("z", "x", "y"), ("z", "y", "x")
    if math.prod(grid.values()) > 16 or tok_count % 128:
        pieces = [(0, tok_count, straight, crossed)]
    else:
        unit = tok_count // 8
        pieces = [
            (0, 3 * unit, first_x, first_y),
            (3 * unit, 3 * unit, straight, crossed),
            (6 * unit, 2 * unit, straight, crossed),
        ]
    parts = []
    for start, rows, order_x, order_o in pieces:
        parts += [(TOKENS, start, rows, order_x), (COTANGENTS, start, rows, order_o)]
    return parts + [(META, 0, 0, first_x), (LOGIT, 0, 0, first_x)]


def routes(grid, order, source, here):
    last = max((i for i, d in enumerate(order) if source[d] != here[d]), default=-1)
    found = []
    if last >= 0:
        d = order[last]
        way = 1 if source[d] < here[d] else -1
        if 0 <= here[d] + way < grid[d]:
            found.append((d, way))
    for d in order[last + 1:]:
        for way in (1, -1):
            if 0 <= here[d] + way < grid[d]:
                found.append((d, way))
    return found


def mean_arrivals(grid, parts, sizes, starts):
    dims = list(grid)
    visits = {d: visit_order(grid[d]) for d in dims}
    nodes = [dict(zip(dims, at)) for at in itertools.product(*[range(grid[d]) for d in dims])]
    queue, free, count, times = [], {}, itertools.count(), {}

    def spread(time, here, part, source):
        for d, way in routes(grid, parts[part][3], source, here):
            key = (tuple(here.values()), d, way)
            begin = max(time, free.get(key, 0.0))
            free[key] = begin + sizes[part] / LINK_RATE
            there = dict(here)
            there[d] += way
            heapq.heappush(queue, (free[key] + LINK_DELAY, next(count), there, part, source))

    for part in range(len(parts)):
        for here in nodes:
            heapq.heappush(queue, (starts[part], next(count), here, part, here))
    while queue:
        time, _, here, part, source = heapq.heappop(queue)
        if source != here:
            key = (part, tuple(visits[d][here[d]].index(source[d]) for d in dims))
            times.setdefault(key, []).append(time)
        spread(time, here, part, source)
    return {key: sum(found) / len(found) for key, found in times.items()}


def make_plan(grid, parts, sizes, starts, chunk_times, send_slot):
    arrivals = sorted((time, key) for key, time in mean_arrivals(grid, parts, sizes, starts).items())
    groups, chunks = len(chunk_times), len(chunk_times[0])
    last = {}
    for index, (_, (part, (jz, jx, jy))) in enumerate(arrivals):
        if parts[part][0] != LOGIT:
            last[jz * grid["x"] + jx] = index
    router_from = groups // 2
    for index, (_, (part, (jz, jx, jy))) in enumerate(arrivals):
        if parts[part][0] == LOGIT:
            user = router_from + (jz * grid["x"] + jx) // 2
            last[user] = max(last.get(user, -1), index)
    slots = [[[] for _ in range(chunks)] for _ in range(groups)]
    late, now, done, held = [], 0.0, 0, []
    for group in range(groups):
        for chunk in range(chunks):
            here = slots[group][chunk]
            sent = (group, chunk) > send_slot
            if sent and held:
                here += held
                held = []
            while done < len(arrivals) and (arrivals[done][0] <= now or done <= last.get(group, -1)):
                time, key = arrivals[done]
                if parts[key[0]][0] == LOGIT and not sent:
                    held.append(key)
                else:
                    here.append(key)
                now = max(now, time)
                done += 1
            now += chunk_times[group][chunk]
    late = held + [key for _, key in arrivals[done:]]
    return slots, late


class Sites:
    def __init__(self, grid, parts):
        self.index = {}
        visits = [range(grid[d]) for d in grid]
        dims = list(grid)
        for part, (_, _, _, order) in enumerate(parts):
            for js in itertools.product(*visits):
                at = dict(zip(dims, js))
                last = max((i for i, d in enumerate(order) if at[d]), default=-1)
                kinds = []
                if last >= 0 and grid[order[last]] > 2:
                    kinds.append((order[last], 0))
                for d in order[last + 1:]:
                    if grid[d] == 2:
                        kinds.append((d, 0))
                    elif grid[d] > 2:
                        kinds += [(d, 1), (d, -1)]
                kinds.append(("core", 0))
                for kind in kinds:
                    self.index[(part, js, kind)] = len(self.index)

    def of(self, part, js):
        return [key[2] for key in self.index if key[0] == part and key[1] == js]


def layer_kernel(copies, flight, cap, grid, parts, sites, slots, late, send_slot, *refs):
    (tok_ref, og_ref, rw_ref, ids_ref, zw_ref, wg_hbm, wd_hbm,
     gu_ref, dn_ref, rout_ref, tg_ref, gx, go,
     wg_ref, wd_ref, xb, ob, rows_x, rows_o, prob_ref, pg_ref, hid, acc_gu, acc_dn,
     logit_ref, small_ref, spot_ref, mref, lref, rgt, back, home_dx, score_ref, home_score,
     wg_sem, wd_sem, own_sem, load_sem, send_sem, recv_sem,
     sc_send, sc_recv, dx_send, dx_recv) = refs
    d = lax.axis_index("dp")
    e = lax.axis_index("expert")
    dims = list(grid)
    top, tok_count = ids_ref.shape
    routed = rw_ref.shape[1]
    hidden_units, width = wd_ref.shape
    rows_group = flight * tok_count
    tile = min(hidden_units, 512)
    wide = min(width, 512)
    gu_rows, dn_rows = gu_ref.shape[1], dn_ref.shape[1]
    core = lax.rem(e, 2)
    my = dict(z=lax.div(d, grid["x"]), x=lax.rem(d, grid["x"]), y=lax.div(e, 2))
    visits = {k: visit_order(grid[k]) for k in dims}
    coord = {
        k: [lookup([visits[k][p][j] for p in range(grid[k])], my[k]) for j in range(grid[k])]
        for k in dims
    }

    def place(at, which):
        return (at["z"] * grid["x"] + at["x"], at["y"] * 2 + which)

    def block_index(at, which):
        dp, expert = place(at, which)
        return dp * flight + expert

    me = block_index(my, core)

    def slice_of(part, index, own=False):
        kind, start, rows, _ = parts[part]
        if kind == META:
            return mref.at[index]
        if kind == LOGIT:
            return lref.at[pl.ds(pl.multiple_of(index * tok_count, tok_count), tok_count), :]
        if own:
            return (tok_ref if kind == TOKENS else og_ref).at[pl.ds(start, rows), :]
        unit = math.gcd(start, tok_count) if start else tok_count
        return (gx if kind == TOKENS else go).at[
            pl.ds(pl.multiple_of(index * tok_count + start, unit), rows), :
        ]

    def arrival(part, index):
        there = slice_of(part, index)
        return pltpu.make_async_remote_copy(
            src_ref=there, dst_ref=there, send_sem=send_sem.at[0],
            recv_sem=recv_sem.at[part, index], device_id=(d, e), device_id_type=MESH,
        )

    def outgoing(part, js, kind):
        at = {k: coord[k][j] for k, j in zip(dims, js)}
        dim, way = kind
        target, guard, which = dict(my), None, core
        if dim == "core":
            which = 1 - core
        elif way == 0 and not at[dim] is my[dim] and js[dims.index(dim)]:
            ahead = my[dim] + jnp.where(at[dim] < my[dim], 1, -1)
            guard = (ahead >= 0) & (ahead < grid[dim])
            target[dim] = ahead
        elif way == 0:
            target[dim] = 1 - my[dim]
        else:
            ahead = my[dim] + way
            guard = (ahead < grid[dim]) if way > 0 else (ahead >= 0)
            target[dim] = ahead
        index = block_index(at, core)
        site = sites.index[(part, js, kind)]
        copy = pltpu.make_async_remote_copy(
            src_ref=slice_of(part, index, own=not any(js)), dst_ref=slice_of(part, index),
            send_sem=send_sem.at[site], recv_sem=recv_sem.at[part, index],
            device_id=place(target, which), device_id_type=MESH,
        )
        return guard, copy

    def each(part, js, act):
        for kind in sites.of(part, js):
            guard, copy = outgoing(part, js, kind)
            if guard is None:
                act(copy)
            else:
                pl.when(guard)(functools.partial(act, copy))

    def handle(event):
        part, js = event
        at = {k: coord[k][j] for k, j in zip(dims, js)}
        arrival(part, block_index(at, core)).wait_recv()
        each(part, js, lambda copy: copy.start())

    home = (0,) * len(dims)

    def start_own(kinds):
        for part, (kind, *_) in enumerate(parts):
            if kind in kinds:
                each(part, home, lambda copy: copy.start())

    barrier = pltpu.get_barrier_semaphore()
    for k in range(1, flight):
        pl.semaphore_signal(
            barrier, inc=1, device_id=(d, lax.rem(e + k, flight)), device_id_type=MESH
        )
    greeted = jnp.int32(flight - 1)
    for k in ("z", "x"):
        for way in (1, -1):
            ahead = my[k] + way
            there = (ahead < grid[k]) if way > 0 else (ahead >= 0)
            greeted = greeted + jnp.where(there, 1, 0)

            @pl.when(there)
            def _():
                target = dict(my)
                target[k] = ahead
                pl.semaphore_signal(
                    barrier, inc=1, device_id=place(target, core), device_id_type=MESH
                )

    load_g = pltpu.make_async_copy(wg_hbm, wg_ref, wg_sem)
    load_d = pltpu.make_async_copy(wd_hbm, wd_ref, wd_sem)
    load_g.start()
    load_d.start()
    mine = pl.ds(pl.multiple_of(me * tok_count, tok_count), tok_count)
    own_x = pltpu.make_async_copy(tok_ref, gx.at[mine, :], own_sem.at[0])
    own_o = pltpu.make_async_copy(og_ref, go.at[mine, :], own_sem.at[1])
    own_x.start()
    own_o.start()
    pl.semaphore_wait(barrier, greeted)
    start_own((TOKENS, COTANGENTS))

    lanes = lax.broadcasted_iota(jnp.int32, (tok_count, routed), 1)

    def column(row):
        return jnp.broadcast_to(row, (routed, tok_count)).T

    ids = [column(ids_ref[k:k + 1, :].astype(F32)).astype(jnp.int32) for k in range(top)]
    choose = [column_ids == lanes for column_ids in ids]
    member = sum(c.astype(F32) for c in choose)
    earlier = lax.broadcasted_iota(jnp.int32, (tok_count, tok_count), 0) > (
        lax.broadcasted_iota(jnp.int32, (tok_count, tok_count), 1)
    )
    rank = jnp.dot(earlier.astype(F32).astype(BF16), member.astype(BF16), preferred_element_type=F32)
    rank = jnp.where(member > 0.0, rank, -1.0)
    logits = jnp.dot(tok_ref[...], rw_ref[...], preferred_element_type=F32)
    chosen = [
        jnp.exp(jnp.sum(jnp.where(c, logits, 0.0), axis=1, keepdims=True)) for c in choose
    ]
    norm = sum(chosen)
    probs = [c / norm for c in chosen]
    weight = jnp.zeros(lanes.shape, F32)
    for k in range(top):
        weight = weight + jnp.where(choose[k], probs[k], 0.0)
    mref[me, 0:flight, :] = rank.T[0:flight, :]
    mref[me, flight:2 * flight, :] = weight.T[0:flight, :]
    start_own((META,))
    logit_ref[...] = logits
    log_total = jnp.log(jnp.sum(jnp.exp(logits), axis=1, keepdims=True))
    small = jnp.where(lanes == top, log_total, column(zw_ref[...]))
    spot = jnp.full(lanes.shape, -1, jnp.int32)
    spots = jnp.where((rank >= 0.0) & (lanes < flight), rank + (lanes * cap).astype(F32) + 1.0, 0.0)
    for k in range(top):
        small = jnp.where(lanes == k, probs[k], small)
        at = jnp.sum(jnp.where(choose[k], spots, 0.0), axis=1, keepdims=True) - 1.0
        spot = jnp.where(lanes == k, at.astype(jnp.int32), spot)
        spot = jnp.where(lanes == top + k, ids[k], spot)
    small_ref[...] = small
    spot_ref[...] = spot
    acc_gu[...] = jnp.zeros_like(acc_gu)
    acc_dn[...] = jnp.zeros_like(acc_dn)
    rgt[...] = jnp.zeros_like(rgt)

    window = acc_dn.shape[0]
    dn_unit = math.gcd(dn_rows, 128)
    dn_start = jnp.minimum(lax.div(d * dn_rows, 128) * 128, hidden_units - window)
    dn_off = pl.multiple_of(d * dn_rows - dn_start, dn_unit)
    dn_start = pl.multiple_of(dn_start, 128)

    def group_at(j):
        jz, jx = lax.div(j, grid["x"]), lax.rem(j, grid["x"])
        z = lookup(sum(visits["z"], []), my["z"] * grid["z"] + jz)
        x = lookup(sum(visits["x"], []), my["x"] * grid["x"] + jx)
        return z * grid["x"] + x

    def wait_sibling(group, kinds):
        for y in range(grid["y"]):
            index = group * flight + 2 * y + 1 - core
            for part, (kind, *_) in enumerate(parts):
                if kind in kinds:
                    arrival(part, index).wait_recv()

    def load_x(group):
        rows = pl.ds(pl.multiple_of(group * rows_group, rows_group), rows_group)
        return pltpu.make_async_copy(gx.at[rows, :], xb, load_sem.at[0])

    def load_o(group):
        rows = pl.ds(pl.multiple_of(group * rows_group, rows_group), rows_group)
        return pltpu.make_async_copy(go.at[rows, :], ob, load_sem.at[1])

    ranks = lax.broadcasted_iota(jnp.int32, (cap, tok_count), 0).astype(F32)

    def gather_rows(group):
        wait_sibling(group, (TOKENS, COTANGENTS, META))
        load_x(group).start()
        load_o(group).start()
        picks = []
        for s in range(flight):
            index = group * flight + s
            pick = mref[index, pl.ds(e, 1), :] == ranks
            part = jnp.where(pick, mref[index, pl.ds(flight + e, 1), :], 0.0)
            prob = jnp.sum(part, axis=1, keepdims=True)
            prob_ref[s * cap:(s + 1) * cap, :] = jnp.broadcast_to(prob, (cap, prob_ref.shape[1]))
            picks.append(pick.astype(F32).astype(BF16))
        load_x(group).wait()
        load_o(group).wait()
        for s in range(flight):
            rows = slice(s * cap, (s + 1) * cap)
            toks = slice(s * tok_count, (s + 1) * tok_count)
            rows_x[rows, :] = jnp.dot(
                picks[s], xb[toks, :], preferred_element_type=F32
            ).astype(BF16)
            rows_o[rows, :] = jnp.dot(
                picks[s], ob[toks, :], preferred_element_type=F32
            ).astype(BF16)

    def hidden_tile(col, own):
        gate = jnp.dot(rows_x[...], wg_ref[:, col:col + tile], preferred_element_type=F32)
        up = jnp.dot(
            rows_x[...], wg_ref[:, hidden_units + col:hidden_units + col + tile],
            preferred_element_type=F32,
        )
        raw = lax.dot_general(
            rows_o[...], wd_ref[col:col + tile, :], (((1,), (1,)), ((), ())),
            preferred_element_type=F32,
        )
        sig = jax.nn.sigmoid(gate)
        active = gate * sig
        hidden = (active * up).astype(BF16)
        hid[:, col:col + tile] = hidden
        grad = prob_ref[:, 0:1] * raw
        pg_ref[:, col:col + tile] = (grad * up * sig * (1.0 + gate * (1.0 - sig))).astype(BF16)
        pg_ref[:, hidden_units + col:hidden_units + col + tile] = (grad * active).astype(BF16)

        @pl.when(own)
        def _():
            part = jnp.sum(raw * hidden.astype(F32), axis=1, keepdims=True)
            part = jnp.broadcast_to(part, score_ref.shape)
            score_ref[...] = part if col == 0 else score_ref[...] + part

    def weight_grads():
        rows_o[...] = (prob_ref[:, 0:1] * rows_o[...].astype(F32)).astype(BF16)
        taken = rows_x[:, pl.ds(pl.multiple_of(d * gu_rows, gu_rows), gu_rows)]
        for col in range(0, 2 * hidden_units, tile):
            acc_gu[:, col:col + tile] += lax.dot_general(
                taken, pg_ref[:, col:col + tile], (((0,), (0,)), ((), ())),
                preferred_element_type=F32,
            )
        taken = hid[:, pl.ds(dn_start, window)]
        for col in range(0, width, wide):
            acc_dn[:, col:col + wide] += lax.dot_general(
                taken, rows_o[:, col:col + wide], (((0,), (0,)), ((), ())),
                preferred_element_type=F32,
            )

    def block(ref, index):
        return ref.at[pl.ds(pl.multiple_of(index * cap, cap), cap), :]

    def give_score(k, source):
        to = lax.rem(e + k, flight)
        return pltpu.make_async_remote_copy(
            src_ref=block(score_ref, to), dst_ref=home_score.at[source],
            send_sem=sc_send.at[k - 1], recv_sem=sc_recv.at[k - 1],
            device_id=(d, to), device_id_type=MESH,
        )

    def give_dx(k, source):
        to = lax.rem(e + k, flight)
        return pltpu.make_async_remote_copy(
            src_ref=block(back, to), dst_ref=block(home_dx, source),
            send_sem=dx_send.at[k - 1], recv_sem=dx_recv.at[k - 1],
            device_id=(d, to), device_id_type=MESH,
        )

    def from_peer(k):
        return lax.rem(e + flight - k, flight)

    def one_hot(k):
        across = lax.broadcasted_iota(jnp.int32, (tok_count, flight * cap), 1)
        return across == spot_ref[:, k:k + 1]

    def row_grads(first, last):
        for col in range(first, last, wide):
            back[:, col:col + wide] = lax.dot_general(
                pg_ref[...], wg_ref[col:col + wide, :], (((1,), (1,)), ((), ())),
                preferred_element_type=F32,
            ).astype(BF16)

    half = width // 2 // wide * wide

    def send_scores():
        for k in range(1, flight):
            give_score(k, e).start()
        home_score[e] = score_ref[pl.ds(pl.multiple_of(e * cap, cap), cap), :]
        row_grads(0, half)

    def send_rows():
        row_grads(half, width)
        for k in range(1, flight):
            give_dx(k, e).start()
        own_rows = pl.ds(pl.multiple_of(e * cap, cap), cap)
        home_dx[own_rows, :] = back[own_rows, :]

    def logit_grads():
        for k in range(1, flight):
            give_score(k, from_peer(k)).wait_recv()
        arrived = home_score[...].reshape(flight * cap, home_score.shape[2])
        logits = logit_ref[...]
        scores = [
            jnp.dot(
                one_hot(k).astype(F32), arrived,
                precision=lax.Precision.HIGHEST, preferred_element_type=F32,
            )
            for k in range(top)
        ]
        probs = [small_ref[:, k:k + 1] for k in range(top)]
        mean = sum(p * q for p, q in zip(probs, scores))
        z_weight = small_ref[:, top + 1:top + 2]
        log_total = small_ref[:, top:top + 1]
        grad = 2.0 * z_weight * log_total * jnp.exp(logits - log_total)
        for k in range(top):
            grad = grad + jnp.where(
                spot_ref[:, top + k:top + k + 1] == lanes, probs[k] * (scores[k] - mean), 0.0
            )
        lref[mine, :] = grad.astype(BF16)
        start_own((LOGIT,))

    def token_grads():
        for k in range(1, flight):
            give_dx(k, from_peer(k)).wait_recv()
        picks = sum(one_hot(k).astype(F32) for k in range(top)).astype(BF16)
        own_lg = lref[mine, :]
        for col in range(0, width, wide):
            total = jnp.dot(picks, home_dx[:, col:col + wide], preferred_element_type=F32)
            total = total + lax.dot_general(
                own_lg, rw_ref[col:col + wide, :], (((1,), (1,)), ((), ())),
                preferred_element_type=F32,
            )
            tg_ref[:, col:col + wide] = total.astype(BF16)

    def router(group):
        wait_sibling(group, (LOGIT,))
        load_x(group).wait()
        rows = pl.ds(pl.multiple_of(group * rows_group, rows_group), rows_group)
        grad = lref[rows, :].astype(F32).T.astype(BF16)
        for col in range(0, width, wide):
            rgt[:, col:col + wide] += jnp.dot(
                grad, xb[:, col:col + wide], preferred_element_type=F32
            )

    tiles = hidden_units // tile

    def step(j, carry):
        group = group_at(j)
        own = j == 0
        late_half = j >= copies // 2
        early = group_at(jnp.maximum(2 * (j - copies // 2), 0))
        second = group_at(jnp.maximum(2 * (j - copies // 2) + 1, 0))

        def events(chunk):
            for k in range(copies):
                if slots[k][chunk]:
                    @pl.when(j == k)
                    def _():
                        for event in slots[k][chunk]:
                            handle(event)

        events(0)

        @pl.when(own)
        def _():
            own_x.wait()
            own_o.wait()

        gather_rows(group)

        @pl.when(late_half)
        def _():
            load_x(early).start()

        @pl.when(own)
        def _():
            load_g.wait()
            load_d.wait()

        for index in range(tiles):
            events(1 + index)
            hidden_tile(index * tile, own)
        events(1 + tiles)
        weight_grads()
        events(2 + tiles)
        pl.when(j == 0)(send_scores)
        pl.when(j == 1)(logit_grads)
        pl.when(j == 2)(token_grads)

        @pl.when(late_half)
        def _():
            router(early)
            load_x(second).start()

        events(3 + tiles)
        pl.when(j == 0)(send_rows)

        @pl.when(late_half)
        def _():
            router(second)

        return carry

    lax.fori_loop(0, copies, step, 0)
    for event in late:
        handle(event)
    gu_ref[0] = acc_gu[...].astype(BF16)
    dn_ref[0] = acc_dn[pl.ds(dn_off, dn_rows), :].astype(BF16)
    rout_ref[...] = rgt[...].T
    for part, js in sorted({key[:2] for key in sites.index}):
        each(part, js, lambda copy: copy.wait_send())
    for k in range(1, flight):
        give_score(k, e).wait_send()
        give_dx(k, e).wait_send()


def finish_kernel(*refs):
    for source, target in zip(refs[:4], refs[4:]):
        target[...] = source[...]


def per_device(tokens, out_grad, z_weight, router_weight, expert_ids, gate_up_weight, down_weight):
    n = lax.axis_size("dp")
    flight = lax.axis_size("expert")
    w_gateup, w_down = gate_up_weight[0], down_weight[0]
    tok_count, width = tokens.shape
    routed = router_weight.shape[1]
    hidden = w_down.shape[0]
    gate_up = w_gateup.shape[1]
    cap = tok_count // 2
    rows = flight * cap
    gu_rows, dn_rows = width // n, hidden // n
    window = min(hidden, (dn_rows + 127) // 128 * 128 + 128)
    if dn_rows % 128 == 0:
        window = dn_rows
    elif dn_rows + (128 - math.gcd(dn_rows, 128)) <= window - 128:
        window -= 128
    grid = grid_of(n, flight)
    parts = make_parts(grid, tok_count)
    sites = Sites(grid, parts)
    sizes = [p[2] * width * 2 for p in parts]
    sizes[-2], sizes[-1] = 8 * flight * tok_count, 2 * tok_count * routed
    starts = [0.0] * (len(parts) - 2) + [4.0, 50.0]
    tiles = hidden // min(hidden, 512)
    base = [2.8] + [2.2] * tiles + [1.8]
    chunk_times = [
        base + ([2.5, 2.5] if j == 0 else [2.0, 0.0] if j < 3 else [0.0, 0.0] if j < n // 2 else [1.3, 1.3])
        for j in range(n)
    ]
    send_slot = (1, 2 + tiles)
    slots, late = make_plan(grid, parts, sizes, starts, chunk_times, send_slot)
    dma = pltpu.SemaphoreType.DMA
    vmem = pl.BlockSpec(memory_space=pltpu.VMEM)
    hbm = pl.BlockSpec(memory_space=pl.ANY)
    shape = jax.ShapeDtypeStruct
    blocks = n * flight
    gate_up_grad, down_grad, router_grad, token_grad, _, _ = pl.pallas_call(
        functools.partial(
            layer_kernel, n, flight, cap, grid, parts, sites, slots, late, send_slot
        ),
        out_shape=(
            shape((1, gu_rows, gate_up), BF16),
            shape((1, dn_rows, width), BF16),
            shape((width, routed), F32),
            shape((tok_count, width), BF16),
            shape((blocks * tok_count, width), BF16),
            shape((blocks * tok_count, width), BF16),
        ),
        in_specs=[vmem] * 5 + [hbm] * 2,
        out_specs=(vmem,) * 4 + (hbm,) * 2,
        scratch_shapes=[
            pltpu.VMEM(w_gateup.shape, BF16),
            pltpu.VMEM(w_down.shape, BF16),
            pltpu.VMEM((flight * tok_count, width), BF16),
            pltpu.VMEM((flight * tok_count, width), BF16),
            pltpu.VMEM((rows, width), BF16),
            pltpu.VMEM((rows, width), BF16),
            pltpu.VMEM((rows, 128), F32),
            pltpu.VMEM((rows, gate_up), BF16),
            pltpu.VMEM((rows, hidden), BF16),
            pltpu.VMEM((gu_rows, gate_up), F32),
            pltpu.VMEM((window, width), F32),
            pltpu.VMEM((tok_count, routed), F32),
            pltpu.VMEM((tok_count, routed), F32),
            pltpu.VMEM((tok_count, routed), jnp.int32),
            pltpu.VMEM((blocks, 2 * flight, tok_count), F32),
            pltpu.VMEM((blocks * tok_count, routed), BF16),
            pltpu.VMEM((routed, width), F32),
            pltpu.VMEM((rows, width), BF16),
            pltpu.VMEM((rows, width), BF16),
            pltpu.VMEM((rows, routed), F32),
            pltpu.VMEM((flight, cap, routed), F32),
            dma, dma, dma((2,)), dma((2,)),
            dma((len(sites.index),)), dma((len(parts), blocks)),
        ] + [dma((flight - 1,))] * 4,
        compiler_params=pltpu.CompilerParams(
            collective_id=0, has_side_effects=True, vmem_limit_bytes=67_000_000
        ),
        name="layer",
    )(
        tokens,
        out_grad,
        router_weight,
        expert_ids.T,
        z_weight[None, :],
        w_gateup,
        w_down,
    )
    results = (token_grad, router_grad, gate_up_grad, down_grad)
    return pl.pallas_call(
        finish_kernel,
        out_shape=tuple(shape(r.shape, r.dtype) for r in results),
        in_specs=[vmem] * 4,
        out_specs=(vmem,) * 4,
        compiler_params=pltpu.CompilerParams(vmem_limit_bytes=16 * 2**20),
        name="finish",
    )(*results)


def solution(mesh):
    return jax.shard_map(
        per_device,
        mesh=mesh,
        in_specs=(
            P(("dp", "expert"), None),
            P(("dp", "expert"), None),
            P(("dp", "expert")),
            P(),
            P(("dp", "expert"), None),
            P("expert", None, None),
            P("expert", None, None),
        ),
        out_specs=(
            P(("dp", "expert"), None),
            P(),
            P("expert", "dp", None),
            P("expert", "dp", None),
        ),
        check_vma=False,
    )
```

```python
import functools
import heapq
import itertools
import math

import jax
import jax.numpy as jnp
from jax import lax
from jax.experimental import pallas as pl
from jax.experimental.pallas import tpu as pltpu
from jax.sharding import PartitionSpec as P

F32 = jnp.float32
BF16 = jnp.bfloat16
MESH = pl.DeviceIdType.MESH
TOKENS, COTANGENTS, META, LOGIT = range(4)
LINK_RATE = 46.6e3
LINK_DELAY = 3.0
EVENT_TIME = 0.25
SEND_TIME = 0.05
LINK_DEPTH = 6.0
META_TIME = 4.0
ALL = "all"


def lookup(table, key):
    value = jnp.int32(0)
    for slot, entry in enumerate(table):
        if entry:
            value = value + jnp.where(key == slot, jnp.int32(entry), jnp.int32(0))
    return value


def grid_of(copies, flight):
    inner = max(k for k in range(1, copies + 1) if copies % k == 0 and k * k <= copies)
    return dict(z=copies // inner, x=inner, y=flight // 2)


def visit_order(size):
    return [
        [i] + sorted((k for k in range(size) if k != i), key=lambda k: (abs(k - i), abs(2 * k + 1 - size)))
        for i in range(size)
    ]


def make_parts(grid, tok_count):
    straight, crossed = ("x", "z", "y"), ("y", "z", "x")
    first_x, first_y = ("z", "x", "y"), ("z", "y", "x")
    if math.prod(grid.values()) > 16 or tok_count % 128:
        pieces = [(0, tok_count, straight, crossed)]
    else:
        unit = tok_count // 8
        pieces = [
            (0, 3 * unit, first_x, first_y),
            (3 * unit, 3 * unit, straight, crossed),
            (6 * unit, 2 * unit, straight, crossed),
        ]
    parts = []
    for start, rows, order_x, order_o in pieces:
        parts += [(TOKENS, start, rows, order_x), (COTANGENTS, start, rows, order_o)]
    return parts + [(META, 0, 0, first_x), (LOGIT, 0, 0, first_x)]


def routes(grid, order, source, here):
    last = max((i for i, d in enumerate(order) if source[d] != here[d]), default=-1)
    found = []
    if last >= 0:
        d = order[last]
        way = 1 if source[d] < here[d] else -1
        if 0 <= here[d] + way < grid[d]:
            found.append((d, way))
    for d in order[last + 1:]:
        for way in (1, -1):
            if 0 <= here[d] + way < grid[d]:
                found.append((d, way))
    return found


def mean_arrivals(grid, parts, sizes):
    dims = list(grid)
    visits = {d: visit_order(grid[d]) for d in dims}
    nodes = [dict(zip(dims, at)) for at in itertools.product(*[range(grid[d]) for d in dims])]
    queue, free, count, times = [], {}, itertools.count(), {}

    def spread(time, here, part, source):
        for d, way in routes(grid, parts[part][3], source, here):
            key = (tuple(here.values()), d, way)
            begin = max(time, free.get(key, 0.0))
            free[key] = begin + sizes[part] / LINK_RATE
            there = dict(here)
            there[d] += way
            heapq.heappush(queue, (free[key] + LINK_DELAY, next(count), there, part, source))

    for part in range(len(parts)):
        for here in nodes:
            heapq.heappush(queue, (0.0, next(count), here, part, here))
    while queue:
        time, _, here, part, source = heapq.heappop(queue)
        if source != here:
            key = (part, tuple(visits[d][here[d]].index(source[d]) for d in dims))
            times.setdefault(key, []).append(time)
        spread(time, here, part, source)
    return {key: sum(found) / len(found) for key, found in times.items()}


def make_plan(grid, parts, sizes, times, share_slot, router_from):
    dims = list(grid)
    visits = {d: visit_order(grid[d]) for d in dims}
    nodes = [dict(zip(dims, at)) for at in itertools.product(*[range(grid[d]) for d in dims])]
    number = {tuple(node.values()): i for i, node in enumerate(nodes)}
    groups, chunks = len(times), len(times[0])
    wanted = {}
    for part, (kind, *_) in enumerate(parts):
        for js in itertools.product(*[range(grid[d]) for d in dims]):
            if any(js):
                key = (kind == LOGIT, js[0] * grid["x"] + js[1])
                wanted.setdefault(key, set()).add((part, js))
    queue, free, count = [], {}, itertools.count()
    ready = [[] for _ in nodes]
    waiting = [{} for _ in nodes]
    seen = [set() for _ in nodes]
    at_slot = [0] * len(nodes)
    asleep = [False] * len(nodes)
    trace = [[] for _ in nodes]
    taken = [[] for _ in nodes]

    def push(time, what, node, *rest):
        heapq.heappush(queue, (round(time, 3), what > 0, next(count), what, node) + rest)

    def offer(node, part, source):
        here = nodes[node]
        js = tuple(visits[d][here[d]].index(source[d]) for d in dims)
        for d, way in routes(grid, parts[part][3], source, here):
            small = parts[part][0] in (META, LOGIT)
            entry = (not small, js[0], part, js, source)
            heapq.heappush(waiting[node].setdefault((d, way), []), entry)

    def own(node, kinds):
        for part, (kind, *_) in enumerate(parts):
            if kind in kinds:
                offer(node, part, nodes[node])

    def startable(node, slot):
        if slot == 0:
            return True
        if slot > groups * chunks:
            return False
        group, chunk = divmod(slot - 1, chunks)
        if chunk == 0:
            for g in range(groups):
                if g not in taken[node] and wanted.get((False, g), set()) <= seen[node]:
                    taken[node].append(g)
                    return True
            return False
        if group >= router_from and chunk >= chunks - 2:
            user = taken[node][2 * (group - router_from) + chunk - chunks + 2]
            return wanted.get((True, user), set()) <= seen[node]
        return True

    for node in range(len(nodes)):
        own(node, (TOKENS, COTANGENTS))
        push(0.0, 1, node)
    while queue:
        time, _, _, what, node, *rest = heapq.heappop(queue)
        here = nodes[node]
        if what == 0:
            part, source = rest
            js = tuple(visits[d][here[d]].index(source[d]) for d in dims)
            heapq.heappush(ready[node], (js[0], time, part, js, source))
        if what in (0, 4):
            if asleep[node]:
                asleep[node] = False
                push(time, 1, node)
            continue
        if what == 2:
            own(node, (META,))
        if what == 3:
            own(node, (LOGIT,))
        slot = at_slot[node]
        if ready[node]:
            _, _, part, js, source = heapq.heappop(ready[node])
            seen[node].add((part, js))
            trace[node].append((slot, (part, js, None)))
            offer(node, part, source)
            push(time + EVENT_TIME, 1, node)
            continue
        open_links = [
            (entries[0], link) for link, entries in waiting[node].items()
            if entries and free.get((node, link), 0.0) - time < LINK_DEPTH
        ]
        if open_links:
            turned = {d: -1 if 2 * here[d] >= grid[d] else 1 for d in dims}
            _, link = min(
                open_links, key=lambda one: (one[0][:4], one[1][0], -one[1][1] * turned[one[1][0]])
            )
            _, _, part, js, source = heapq.heappop(waiting[node][link])
            trace[node].append((slot, (part, js, link)))
            end = max(time, free.get((node, link), 0.0)) + sizes[part] / LINK_RATE
            free[(node, link)] = end
            there = dict(here)
            there[link[0]] += link[1]
            push(end + LINK_DELAY, 0, number[tuple(there.values())], part, source)
            push(time + SEND_TIME, 1, node)
            continue
        if startable(node, slot):
            at_slot[node] += 1
            if slot == 0:
                push(time + META_TIME, 2, node)
            else:
                group, chunk = divmod(slot - 1, chunks)
                push(time + times[group][chunk], 3 if slot == share_slot else 1, node)
            continue
        asleep[node] = True
        wake = [free[(node, link)] - LINK_DEPTH for link, entries in waiting[node].items() if entries]
        if wake:
            push(max(min(wake), time) + 0.01, 4, node)
    return nodes, trace, taken, time


def mirrored(grid, node, plan):
    flips = {d for d in grid if 2 * node[d] >= grid[d]}
    return [
        (at, (part, js, link and (link[0], -link[1] if link[0] in flips else link[1])))
        for at, (part, js, link) in plan
    ]


def make_slots(grid, parts, sizes, times, share_slot, router_from):
    nodes, trace, taken, _ = make_plan(grid, parts, sizes, times, share_slot, router_from)
    groups = len(times)
    flat = [mirrored(grid, node, plan) for node, plan in zip(nodes, trace)]
    kinds = [min(node["z"], grid["z"] - 1 - node["z"]) for node in nodes]
    known = sorted(set(kinds))
    firsts = [kinds.index(kind) for kind in known]
    same = all(
        sorted(map(repr, flat[i])) == sorted(map(repr, flat[firsts[known.index(kind)]]))
        and taken[i] == taken[firsts[known.index(kind)]]
        for i, kind in enumerate(kinds)
    )
    if same and max(grid["x"], grid["y"]) <= 2:
        table = [known.index(min(z, grid["z"] - 1 - z)) for z in range(grid["z"])]
        plans = [flat[i] for i in firsts]
        orders = [taken[i] for i in firsts]
    else:
        table, orders = [0] * grid["z"], [list(range(groups))]
        arrivals = mean_arrivals(grid, parts, sizes)
        plan = []
        for kinds_now, at in (((TOKENS, COTANGENTS), 0), ((META,), 1), ((LOGIT,), share_slot + 1)):
            for part, (kind, *_) in enumerate(parts):
                if kind in kinds_now:
                    plan.append((at, (part, (0, 0, 0), ALL)))
        for _, (part, js) in sorted((time, key) for key, time in arrivals.items()):
            at = share_slot + 1 if parts[part][0] == LOGIT else 1
            plan += [(at, (part, js, None)), (at, (part, js, ALL))]
        plans = [plan]
    slots = []
    for plan in plans:
        found = {}
        for at, action in plan:
            found.setdefault(at, []).append(action)
        slots.append(found)
    return table, slots, orders


class Sites:
    def __init__(self, grid, parts):
        self.index = {}
        visits = [range(grid[d]) for d in grid]
        dims = list(grid)
        for part, (_, _, _, order) in enumerate(parts):
            for js in itertools.product(*visits):
                at = dict(zip(dims, js))
                last = max((i for i, d in enumerate(order) if at[d]), default=-1)
                kinds = []
                if last >= 0 and grid[order[last]] > 2:
                    kinds.append((order[last], 0))
                for d in order[last + 1:]:
                    if grid[d] == 2:
                        kinds.append((d, 0))
                    elif grid[d] > 2:
                        kinds += [(d, 1), (d, -1)]
                kinds.append(("core", 0))
                for kind in kinds:
                    self.index[(part, js, kind)] = len(self.index)

    def of(self, part, js):
        return [key[2] for key in self.index if key[0] == part and key[1] == js]


def layer_kernel(copies, flight, cap, grid, parts, sites, table, slots, orders, chunks, *refs):
    (tok_ref, og_ref, rw_ref, ids_ref, zw_ref, wg_hbm, wd_hbm,
     gu_ref, dn_ref, rout_ref, tg_ref, gx, go,
     wg_ref, wd_ref, xb, ob, rows_x, rows_o, prob_ref, gate_ref, up_ref, pg_ref, hid, acc_gu, acc_dn,
     logit_ref, small_ref, spot_ref, mref, lref, rgt, back, home_dx, score_ref, home_score,
     wg_sem, wd_sem, own_sem, load_sem, send_sem, recv_sem,
     sc_send, sc_recv, dx_send, dx_recv) = refs
    d = lax.axis_index("dp")
    e = lax.axis_index("expert")
    dims = list(grid)
    top, tok_count = ids_ref.shape
    routed = rw_ref.shape[1]
    hidden_units, width = wd_ref.shape
    rows_group = flight * tok_count
    tile = min(hidden_units, 512)
    wide = min(width, 512)
    gu_rows, dn_rows = gu_ref.shape[1], dn_ref.shape[1]
    core = lax.rem(e, 2)
    my = dict(z=lax.div(d, grid["x"]), x=lax.rem(d, grid["x"]), y=lax.div(e, 2))
    visits = {k: visit_order(grid[k]) for k in dims}
    coord = {
        k: [lookup([visits[k][p][j] for p in range(grid[k])], my[k]) for j in range(grid[k])]
        for k in dims
    }

    def place(at, which):
        return (at["z"] * grid["x"] + at["x"], at["y"] * 2 + which)

    def block_index(at, which):
        dp, expert = place(at, which)
        return dp * flight + expert

    me = block_index(my, core)
    my_kind = lookup(table, my["z"])
    my_flip = 2 * my["z"] >= grid["z"]

    def slice_of(part, index, own=False):
        kind, start, rows, _ = parts[part]
        if kind == META:
            return mref.at[index]
        if kind == LOGIT:
            return lref.at[pl.ds(pl.multiple_of(index * tok_count, tok_count), tok_count), :]
        if own:
            return (tok_ref if kind == TOKENS else og_ref).at[pl.ds(start, rows), :]
        unit = math.gcd(start, tok_count) if start else tok_count
        return (gx if kind == TOKENS else go).at[
            pl.ds(pl.multiple_of(index * tok_count + start, unit), rows), :
        ]

    def arrival(part, index):
        there = slice_of(part, index)
        return pltpu.make_async_remote_copy(
            src_ref=there, dst_ref=there, send_sem=send_sem.at[0],
            recv_sem=recv_sem.at[part, index], device_id=(d, e), device_id_type=MESH,
        )

    def outgoing(part, js, kind):
        at = {k: coord[k][j] for k, j in zip(dims, js)}
        dim, way = kind
        target, guard, which = dict(my), None, core
        if dim == "core":
            which = 1 - core
        elif way == 0 and not at[dim] is my[dim] and js[dims.index(dim)]:
            ahead = my[dim] + jnp.where(at[dim] < my[dim], 1, -1)
            guard = (ahead >= 0) & (ahead < grid[dim])
            target[dim] = ahead
        elif way == 0:
            target[dim] = 1 - my[dim]
        else:
            ahead = my[dim] + way
            guard = (ahead < grid[dim]) if way > 0 else (ahead >= 0)
            target[dim] = ahead
        index = block_index(at, core)
        site = sites.index[(part, js, kind)]
        copy = pltpu.make_async_remote_copy(
            src_ref=slice_of(part, index, own=not any(js)), dst_ref=slice_of(part, index),
            send_sem=send_sem.at[site], recv_sem=recv_sem.at[part, index],
            device_id=place(target, which), device_id_type=MESH,
        )
        return guard, copy

    def each(part, js, act):
        for kind in sites.of(part, js):
            guard, copy = outgoing(part, js, kind)
            if guard is None:
                act(copy)
            else:
                pl.when(guard)(functools.partial(act, copy))

    def launch(part, js, wanted):
        for kind in sites.of(part, js):
            if not wanted(kind):
                continue
            guard, copy = outgoing(part, js, kind)
            if guard is None:
                copy.start()
            else:
                pl.when(guard)(copy.start)

    def handle(action, flipped):
        part, js, link = action
        if link is None:
            at = {k: coord[k][j] for k, j in zip(dims, js)}
            arrival(part, block_index(at, core)).wait_recv()
            launch(part, js, lambda kind: kind[0] == "core")
        elif link == ALL:
            launch(part, js, lambda kind: kind[0] != "core")
        elif grid[link[0]] > 2 and not js[dims.index(link[0])]:
            pl.when(flipped)(lambda: launch(part, js, lambda kind: kind == (link[0], -link[1])))
            pl.when(~flipped)(lambda: launch(part, js, lambda kind: kind == link))
        else:
            launch(part, js, lambda kind: kind[0] == link[0])

    def run_actions(slot, when=None):
        for kind, found in enumerate(slots):
            if slot in found:
                here = my_kind == kind
                if when is not None:
                    here = here & when

                @pl.when(here)
                def _():
                    for action in found[slot]:
                        handle(action, my_flip)

    home = (0,) * len(dims)

    def start_own(kinds):
        for part, (kind, *_) in enumerate(parts):
            if kind in kinds:
                launch(part, home, lambda kind: kind[0] == "core")

    barrier = pltpu.get_barrier_semaphore()
    for k in range(1, flight):
        pl.semaphore_signal(
            barrier, inc=1, device_id=(d, lax.rem(e + k, flight)), device_id_type=MESH
        )
    greeted = jnp.int32(flight - 1)
    for k in ("z", "x"):
        for way in (1, -1):
            ahead = my[k] + way
            there = (ahead < grid[k]) if way > 0 else (ahead >= 0)
            greeted = greeted + jnp.where(there, 1, 0)

            @pl.when(there)
            def _():
                target = dict(my)
                target[k] = ahead
                pl.semaphore_signal(
                    barrier, inc=1, device_id=place(target, core), device_id_type=MESH
                )

    load_g = pltpu.make_async_copy(wg_hbm, wg_ref, wg_sem)
    load_d = pltpu.make_async_copy(wd_hbm, wd_ref, wd_sem)
    load_g.start()
    load_d.start()
    mine = pl.ds(pl.multiple_of(me * tok_count, tok_count), tok_count)
    own_x = pltpu.make_async_copy(tok_ref, gx.at[mine, :], own_sem.at[0])
    own_o = pltpu.make_async_copy(og_ref, go.at[mine, :], own_sem.at[1])
    own_x.start()
    own_o.start()
    pl.semaphore_wait(barrier, greeted)
    run_actions(0)
    start_own((TOKENS, COTANGENTS))

    lanes = lax.broadcasted_iota(jnp.int32, (tok_count, routed), 1)

    def column(row):
        return jnp.broadcast_to(row, (routed, tok_count)).T

    ids = [column(ids_ref[k:k + 1, :].astype(F32)).astype(jnp.int32) for k in range(top)]
    choose = [column_ids == lanes for column_ids in ids]
    member = sum(c.astype(F32) for c in choose)
    earlier = lax.broadcasted_iota(jnp.int32, (tok_count, tok_count), 0) > (
        lax.broadcasted_iota(jnp.int32, (tok_count, tok_count), 1)
    )
    rank = jnp.dot(earlier.astype(F32).astype(BF16), member.astype(BF16), preferred_element_type=F32)
    rank = jnp.where(member > 0.0, rank, -1.0)
    logits = jnp.dot(tok_ref[...], rw_ref[...], preferred_element_type=F32)
    chosen = [
        jnp.exp(jnp.sum(jnp.where(c, logits, 0.0), axis=1, keepdims=True)) for c in choose
    ]
    norm = sum(chosen)
    probs = [c / norm for c in chosen]
    weight = jnp.zeros(lanes.shape, F32)
    for k in range(top):
        weight = weight + jnp.where(choose[k], probs[k], 0.0)
    mref[me, 0:flight, :] = rank.T[0:flight, :]
    mref[me, flight:2 * flight, :] = weight.T[0:flight, :]
    start_own((META,))
    logit_ref[...] = logits
    log_total = jnp.log(jnp.sum(jnp.exp(logits), axis=1, keepdims=True))
    small = jnp.where(lanes == top, log_total, column(zw_ref[...]))
    spot = jnp.full(lanes.shape, -1, jnp.int32)
    spots = jnp.where((rank >= 0.0) & (lanes < flight), rank + (lanes * cap).astype(F32) + 1.0, 0.0)
    for k in range(top):
        small = jnp.where(lanes == k, probs[k], small)
        at = jnp.sum(jnp.where(choose[k], spots, 0.0), axis=1, keepdims=True) - 1.0
        spot = jnp.where(lanes == k, at.astype(jnp.int32), spot)
        spot = jnp.where(lanes == top + k, ids[k], spot)
    small_ref[...] = small
    spot_ref[...] = spot
    acc_gu[...] = jnp.zeros_like(acc_gu)
    acc_dn[...] = jnp.zeros_like(acc_dn)
    rgt[...] = jnp.zeros_like(rgt)

    window = acc_dn.shape[0]
    dn_unit = math.gcd(dn_rows, 128)
    dn_start = jnp.minimum(lax.div(d * dn_rows, 128) * 128, hidden_units - window)
    dn_off = pl.multiple_of(d * dn_rows - dn_start, dn_unit)
    dn_start = pl.multiple_of(dn_start, 128)

    def group_at(j):
        g = lookup(sum(orders, []), my_kind * copies + j)
        jz, jx = lax.div(g, grid["x"]), lax.rem(g, grid["x"])
        z = lookup(sum(visits["z"], []), my["z"] * grid["z"] + jz)
        x = lookup(sum(visits["x"], []), my["x"] * grid["x"] + jx)
        return z * grid["x"] + x

    def wait_sibling(group, kinds):
        for y in range(grid["y"]):
            index = group * flight + 2 * y + 1 - core
            for part, (kind, *_) in enumerate(parts):
                if kind in kinds:
                    arrival(part, index).wait_recv()

    def load_x(group):
        rows = pl.ds(pl.multiple_of(group * rows_group, rows_group), rows_group)
        return pltpu.make_async_copy(gx.at[rows, :], xb, load_sem.at[0])

    def load_o(group):
        rows = pl.ds(pl.multiple_of(group * rows_group, rows_group), rows_group)
        return pltpu.make_async_copy(go.at[rows, :], ob, load_sem.at[1])

    ranks = lax.broadcasted_iota(jnp.int32, (2 * cap, 2 * tok_count), 0).astype(F32)

    def pair_rank(group, pair):
        index = group * flight + 2 * pair
        first = mref[index, pl.ds(e, 1), :]
        second = mref[index + 1, pl.ds(e, 1), :]
        second = jnp.where(second >= 0.0, second + float(cap), -1.0)
        return jnp.concatenate([first, second], axis=1) == ranks

    def pick_rows(group, source, target):
        for pair in range(flight // 2):
            picks = pair_rank(group, pair).astype(F32).astype(BF16)
            target[pair * 2 * cap:(pair + 1) * 2 * cap, :] = jnp.dot(
                picks, source[pair * 2 * tok_count:(pair + 1) * 2 * tok_count, :],
                preferred_element_type=F32,
            ).astype(BF16)

    def gather_x(group):
        wait_sibling(group, (TOKENS, COTANGENTS, META))
        load_x(group).start()
        load_o(group).start()
        for pair in range(flight // 2):
            index = group * flight + 2 * pair
            weights = jnp.concatenate(
                [mref[index + i, pl.ds(flight + e, 1), :] for i in range(2)], axis=1
            )
            part = jnp.where(pair_rank(group, pair), weights, 0.0)
            prob = jnp.sum(part, axis=1, keepdims=True)
            prob_ref[pair * 2 * cap:(pair + 1) * 2 * cap, :] = jnp.broadcast_to(
                prob, (2 * cap, prob_ref.shape[1])
            )
        load_x(group).wait()
        pick_rows(group, xb, rows_x)

    def gather_o(group):
        load_o(group).wait()
        pick_rows(group, ob, rows_o)

    def gate_tile(col):
        gate_ref[...] = jnp.dot(
            rows_x[...], wg_ref[:, col:col + tile], preferred_element_type=F32
        )

    def up_tile(col):
        up_ref[...] = jnp.dot(
            rows_x[...], wg_ref[:, hidden_units + col:hidden_units + col + tile],
            preferred_element_type=F32,
        )

    def hidden_tile(col, own):
        gate, up = gate_ref[...], up_ref[...]
        raw = lax.dot_general(
            rows_o[...], wd_ref[col:col + tile, :], (((1,), (1,)), ((), ())),
            preferred_element_type=F32,
        )
        sig = jax.nn.sigmoid(gate)
        active = gate * sig
        hidden = (active * up).astype(BF16)
        hid[:, col:col + tile] = hidden
        grad = prob_ref[:, 0:1] * raw
        pg_ref[:, col:col + tile] = (grad * up * sig * (1.0 + gate * (1.0 - sig))).astype(BF16)
        pg_ref[:, hidden_units + col:hidden_units + col + tile] = (grad * active).astype(BF16)

        @pl.when(own)
        def _():
            part = jnp.sum(raw * hidden.astype(F32), axis=1, keepdims=True)
            part = jnp.broadcast_to(part, score_ref.shape)
            score_ref[...] = part if col == 0 else score_ref[...] + part

    def up_grads():
        rows_o[...] = (prob_ref[:, 0:1] * rows_o[...].astype(F32)).astype(BF16)
        taken = rows_x[:, pl.ds(pl.multiple_of(d * gu_rows, gu_rows), gu_rows)]
        for col in range(0, 2 * hidden_units, tile):
            acc_gu[:, col:col + tile] += lax.dot_general(
                taken, pg_ref[:, col:col + tile], (((0,), (0,)), ((), ())),
                preferred_element_type=F32,
            )

    def down_grads():
        taken = hid[:, pl.ds(dn_start, window)]
        for col in range(0, width, wide):
            acc_dn[:, col:col + wide] += lax.dot_general(
                taken, rows_o[:, col:col + wide], (((0,), (0,)), ((), ())),
                preferred_element_type=F32,
            )

    def block(ref, index):
        return ref.at[pl.ds(pl.multiple_of(index * cap, cap), cap), :]

    def give_score(k, source):
        to = lax.rem(e + k, flight)
        return pltpu.make_async_remote_copy(
            src_ref=block(score_ref, to), dst_ref=home_score.at[source],
            send_sem=sc_send.at[k - 1], recv_sem=sc_recv.at[k - 1],
            device_id=(d, to), device_id_type=MESH,
        )

    def give_dx(k, source):
        to = lax.rem(e + k, flight)
        return pltpu.make_async_remote_copy(
            src_ref=block(back, to), dst_ref=block(home_dx, source),
            send_sem=dx_send.at[k - 1], recv_sem=dx_recv.at[k - 1],
            device_id=(d, to), device_id_type=MESH,
        )

    def from_peer(k):
        return lax.rem(e + flight - k, flight)

    def one_hot(k):
        across = lax.broadcasted_iota(jnp.int32, (tok_count, flight * cap), 1)
        return across == spot_ref[:, k:k + 1]

    def row_grads(first, last):
        for col in range(first, last, wide):
            back[:, col:col + wide] = lax.dot_general(
                pg_ref[...], wg_ref[col:col + wide, :], (((1,), (1,)), ((), ())),
                preferred_element_type=F32,
            ).astype(BF16)

    half = width // 2 // wide * wide

    def send_scores():
        for k in range(1, flight):
            give_score(k, e).start()
        home_score[e] = score_ref[pl.ds(pl.multiple_of(e * cap, cap), cap), :]
        row_grads(0, half)

    def send_rows():
        row_grads(half, width)
        for k in range(1, flight):
            give_dx(k, e).start()
        own_rows = pl.ds(pl.multiple_of(e * cap, cap), cap)
        home_dx[own_rows, :] = back[own_rows, :]

    def logit_grads():
        for k in range(1, flight):
            give_score(k, from_peer(k)).wait_recv()
        arrived = home_score[...].reshape(flight * cap, home_score.shape[2])
        logits = logit_ref[...]
        scores = [
            jnp.dot(
                one_hot(k).astype(F32), arrived,
                precision=lax.Precision.HIGHEST, preferred_element_type=F32,
            )
            for k in range(top)
        ]
        probs = [small_ref[:, k:k + 1] for k in range(top)]
        mean = sum(p * q for p, q in zip(probs, scores))
        z_weight = small_ref[:, top + 1:top + 2]
        log_total = small_ref[:, top:top + 1]
        grad = 2.0 * z_weight * log_total * jnp.exp(logits - log_total)
        for k in range(top):
            grad = grad + jnp.where(
                spot_ref[:, top + k:top + k + 1] == lanes, probs[k] * (scores[k] - mean), 0.0
            )
        lref[mine, :] = grad.astype(BF16)
        start_own((LOGIT,))

    def token_grads():
        for k in range(1, flight):
            give_dx(k, from_peer(k)).wait_recv()
        picks = sum(one_hot(k).astype(F32) for k in range(top)).astype(BF16)
        own_lg = lref[mine, :]
        for col in range(0, width, wide):
            total = jnp.dot(picks, home_dx[:, col:col + wide], preferred_element_type=F32)
            total = total + lax.dot_general(
                own_lg, rw_ref[col:col + wide, :], (((1,), (1,)), ((), ())),
                preferred_element_type=F32,
            )
            tg_ref[:, col:col + wide] = total.astype(BF16)

    def router(group):
        wait_sibling(group, (LOGIT,))
        load_x(group).wait()
        rows = pl.ds(pl.multiple_of(group * rows_group, rows_group), rows_group)
        grad = lref[rows, :].astype(F32).T.astype(BF16)
        for col in range(0, width, wide):
            rgt[:, col:col + wide] += jnp.dot(
                grad, xb[:, col:col + wide], preferred_element_type=F32
            )

    tiles = hidden_units // tile

    def step(j, carry):
        group = group_at(j)
        own = j == 0
        late_half = j >= copies // 2
        early = group_at(jnp.maximum(2 * (j - copies // 2), 0))
        second = group_at(jnp.maximum(2 * (j - copies // 2) + 1, 0))

        spot_now = [0]

        def then(run):
            chunk = spot_now[0]
            spot_now[0] += 1
            for k in range(copies):
                run_actions(1 + k * chunks + chunk, j == k)
            run()

        def first_rows():
            @pl.when(own)
            def _():
                own_x.wait()
                own_o.wait()

            gather_x(group)

            @pl.when(late_half)
            def _():
                load_x(early).start()

            @pl.when(own)
            def _():
                load_g.wait()
                load_d.wait()

        then(first_rows)
        then(lambda: gather_o(group))
        for index in range(tiles):
            then(functools.partial(gate_tile, index * tile))
            then(functools.partial(up_tile, index * tile))
            then(functools.partial(hidden_tile, index * tile, own))
        then(up_grads)
        then(down_grads)

        def special():
            pl.when(j == 0)(send_scores)
            pl.when(j == 1)(logit_grads)
            pl.when(j == 2)(token_grads)

            @pl.when(late_half)
            def _():
                router(early)
                load_x(second).start()

        def special_late():
            pl.when(j == 0)(send_rows)

            @pl.when(late_half)
            def _():
                router(second)

        then(special)
        then(special_late)
        return carry

    lax.fori_loop(0, copies, step, 0)
    run_actions(1 + copies * chunks)
    gu_ref[0] = acc_gu[...].astype(BF16)
    dn_ref[0] = acc_dn[pl.ds(dn_off, dn_rows), :].astype(BF16)
    rout_ref[...] = rgt[...].T
    for part, js in sorted({key[:2] for key in sites.index}):
        each(part, js, lambda copy: copy.wait_send())
    for k in range(1, flight):
        give_score(k, e).wait_send()
        give_dx(k, e).wait_send()


def finish_kernel(*refs):
    sources, targets, holds, sems = refs[:4], refs[4:8], refs[8:12], refs[12]
    takes = [
        pltpu.make_async_copy(source, hold, sems.at[i])
        for i, (source, hold) in enumerate(zip(sources, holds))
    ]
    gives = [
        pltpu.make_async_copy(hold, target, sems.at[4 + i])
        for i, (hold, target) in enumerate(zip(holds, targets))
    ]
    for take in takes:
        take.start()
    for take, give in zip(takes, gives):
        take.wait()
        give.start()
    for give in gives:
        give.wait()


def per_device(tokens, out_grad, z_weight, router_weight, expert_ids, gate_up_weight, down_weight):
    n = lax.axis_size("dp")
    flight = lax.axis_size("expert")
    w_gateup, w_down = gate_up_weight[0], down_weight[0]
    tok_count, width = tokens.shape
    routed = router_weight.shape[1]
    hidden = w_down.shape[0]
    gate_up = w_gateup.shape[1]
    cap = tok_count // 2
    rows = flight * cap
    gu_rows, dn_rows = width // n, hidden // n
    window = min(hidden, (dn_rows + 127) // 128 * 128 + 128)
    if dn_rows % 128 == 0:
        window = dn_rows
    elif dn_rows + (128 - math.gcd(dn_rows, 128)) <= window - 128:
        window -= 128
    grid = grid_of(n, flight)
    parts = make_parts(grid, tok_count)
    sites = Sites(grid, parts)
    sizes = [p[2] * width * 2 for p in parts]
    sizes[-2], sizes[-1] = 8 * flight * tok_count, 2 * tok_count * routed
    tiles = hidden // min(hidden, 512)
    base = [1.9, 1.0] + [0.57, 0.57, 0.75] * tiles + [0.75, 0.55]
    chunk_times = [
        base + ([2.0, 2.0] if j == 0 else [1.6, 0.1] if j < 3 else [0.1, 0.1] if j < n // 2 else [1.3, 1.3])
        for j in range(n)
    ]
    chunks = len(base) + 2
    share_slot = 1 + chunks + len(base)
    table, slots, orders = make_slots(grid, parts, sizes, chunk_times, share_slot, n // 2)
    dma = pltpu.SemaphoreType.DMA
    vmem = pl.BlockSpec(memory_space=pltpu.VMEM)
    hbm = pl.BlockSpec(memory_space=pl.ANY)
    shape = jax.ShapeDtypeStruct
    blocks = n * flight
    gate_up_grad, down_grad, router_grad, token_grad, _, _ = pl.pallas_call(
        functools.partial(
            layer_kernel, n, flight, cap, grid, parts, sites, table, slots, orders, chunks
        ),
        out_shape=(
            shape((1, gu_rows, gate_up), BF16),
            shape((1, dn_rows, width), BF16),
            shape((width, routed), F32),
            shape((tok_count, width), BF16),
            shape((blocks * tok_count, width), BF16),
            shape((blocks * tok_count, width), BF16),
        ),
        in_specs=[vmem] * 5 + [hbm] * 2,
        out_specs=(vmem,) * 4 + (hbm,) * 2,
        scratch_shapes=[
            pltpu.VMEM(w_gateup.shape, BF16),
            pltpu.VMEM(w_down.shape, BF16),
            pltpu.VMEM((flight * tok_count, width), BF16),
            pltpu.VMEM((flight * tok_count, width), BF16),
            pltpu.VMEM((rows, width), BF16),
            pltpu.VMEM((rows, width), BF16),
            pltpu.VMEM((rows, 128), F32),
            pltpu.VMEM((rows, min(hidden, 512)), F32),
            pltpu.VMEM((rows, min(hidden, 512)), F32),
            pltpu.VMEM((rows, gate_up), BF16),
            pltpu.VMEM((rows, hidden), BF16),
            pltpu.VMEM((gu_rows, gate_up), F32),
            pltpu.VMEM((window, width), F32),
            pltpu.VMEM((tok_count, routed), F32),
            pltpu.VMEM((tok_count, routed), F32),
            pltpu.VMEM((tok_count, routed), jnp.int32),
            pltpu.VMEM((blocks, 2 * flight, tok_count), F32),
            pltpu.VMEM((blocks * tok_count, routed), BF16),
            pltpu.VMEM((routed, width), F32),
            pltpu.VMEM((rows, width), BF16),
            pltpu.VMEM((rows, width), BF16),
            pltpu.VMEM((rows, routed), F32),
            pltpu.VMEM((flight, cap, routed), F32),
            dma, dma, dma((2,)), dma((2,)),
            dma((len(sites.index),)), dma((len(parts), blocks)),
        ] + [dma((flight - 1,))] * 4,
        compiler_params=pltpu.CompilerParams(
            collective_id=0, has_side_effects=True, vmem_limit_bytes=67_000_000
        ),
        name="layer",
    )(
        tokens,
        out_grad,
        router_weight,
        expert_ids.T,
        z_weight[None, :],
        w_gateup,
        w_down,
    )
    results = (token_grad, router_grad, gate_up_grad, down_grad)
    return pl.pallas_call(
        finish_kernel,
        out_shape=tuple(shape(r.shape, r.dtype) for r in results),
        in_specs=[hbm] * 4,
        out_specs=(hbm,) * 4,
        scratch_shapes=[pltpu.VMEM(r.shape, r.dtype) for r in results] + [dma((8,))],
        compiler_params=pltpu.CompilerParams(vmem_limit_bytes=67_000_000),
        name="finish",
    )(*results)


def solution(mesh):
    return jax.shard_map(
        per_device,
        mesh=mesh,
        in_specs=(
            P(("dp", "expert"), None),
            P(("dp", "expert"), None),
            P(("dp", "expert")),
            P(),
            P(("dp", "expert"), None),
            P("expert", None, None),
            P("expert", None, None),
        ),
        out_specs=(
            P(("dp", "expert"), None),
            P(),
            P("expert", "dp", None),
            P("expert", "dp", None),
        ),
        check_vma=False,
    )
```

```python
import functools
import heapq
import itertools
import math

import jax
import jax.numpy as jnp
from jax import lax
from jax.experimental import pallas as pl
from jax.experimental.pallas import tpu as pltpu
from jax.sharding import PartitionSpec as P

F32 = jnp.float32
BF16 = jnp.bfloat16
MESH = pl.DeviceIdType.MESH
TOKENS, BLOCK, META, LOGIT = range(4)
LINK_RATE = 46.6e3
LINK_DELAY = 3.0
EVENT_TIME = 0.25
SEND_TIME = 0.05
LINK_DEPTH = 12.0
META_TIME = 4.0
ALL, CORE = "all", "core"


def lookup(table, key):
    value = jnp.int32(0)
    for slot, entry in enumerate(table):
        if entry:
            value = value + jnp.where(key == slot, jnp.int32(entry), jnp.int32(0))
    return value


def grid_of(copies, flight):
    inner = max(k for k in range(1, copies + 1) if copies % k == 0 and k * k <= copies)
    return dict(z=copies // inner, x=inner, y=flight // 2)


def visit_order(size):
    return [
        [i] + sorted((k for k in range(size) if k != i), key=lambda k: (abs(k - i), abs(2 * k + 1 - size)))
        for i in range(size)
    ]


def make_parts(grid, tok_count):
    straight, crossed = ("x", "z", "y"), ("y", "z", "x")
    first_x, first_y = ("z", "x", "y"), ("z", "y", "x")
    if math.prod(grid.values()) > 16 or tok_count % 64:
        half = tok_count // 2
        parts = [(TOKENS, 0, half, straight), (TOKENS, half, half, crossed)]
    else:
        unit = tok_count // 4
        parts = [
            (TOKENS, i * unit, unit, order)
            for i, order in enumerate((first_x, first_y, straight, crossed))
        ]
    return parts + [(BLOCK, 0, 0, first_x), (META, 0, 0, first_x), (LOGIT, 0, 0, first_x)]


def routes(grid, order, source, here):
    last = max((i for i, d in enumerate(order) if source[d] != here[d]), default=-1)
    found = []
    if last >= 0:
        d = order[last]
        way = 1 if source[d] < here[d] else -1
        if 0 <= here[d] + way < grid[d]:
            found.append((d, way))
    for d in order[last + 1:]:
        for way in (1, -1):
            if 0 <= here[d] + way < grid[d]:
                found.append((d, way))
    return found


def mean_arrivals(grid, parts, sizes):
    dims = list(grid)
    visits = {d: visit_order(grid[d]) for d in dims}
    nodes = [dict(zip(dims, at)) for at in itertools.product(*[range(grid[d]) for d in dims])]
    queue, free, count, times = [], {}, itertools.count(), {}

    def spread(time, here, part, source):
        for d, way in routes(grid, parts[part][3], source, here):
            key = (tuple(here.values()), d, way)
            begin = max(time, free.get(key, 0.0))
            free[key] = begin + sizes[part] / LINK_RATE
            there = dict(here)
            there[d] += way
            heapq.heappush(queue, (free[key] + LINK_DELAY, next(count), there, part, source))

    for part in range(len(parts)):
        for here in nodes:
            if parts[part][0] == BLOCK:
                continue
            heapq.heappush(queue, (0.0, next(count), here, part, here))
    while queue:
        time, _, here, part, source = heapq.heappop(queue)
        if source != here:
            key = (part, tuple(visits[d][here[d]].index(source[d]) for d in dims))
            times.setdefault(key, []).append(time)
        spread(time, here, part, source)
    return {key: sum(found) / len(found) for key, found in times.items()}


def make_plan(grid, parts, sizes, times, share_slot, router_from):
    dims = list(grid)
    visits = {d: visit_order(grid[d]) for d in dims}
    nodes = [dict(zip(dims, at)) for at in itertools.product(*[range(grid[d]) for d in dims])]
    number = {tuple(node.values()): i for i, node in enumerate(nodes)}
    groups, chunks = len(times), len(times[0])
    wanted = {}
    whole = sum(kind == TOKENS for kind, *_ in parts)
    for part, (kind, *_) in enumerate(parts):
        for js in itertools.product(*[range(grid[d]) for d in dims]):
            if any(js) and kind != BLOCK:
                key = (kind == LOGIT, js[0] * grid["x"] + js[1])
                wanted.setdefault(key, set()).add((part, js))
    queue, free, count = [], {}, itertools.count()
    ready = [[] for _ in nodes]
    waiting = [{} for _ in nodes]
    seen = [set() for _ in nodes]
    at_slot = [0] * len(nodes)
    asleep = [False] * len(nodes)
    trace = [[] for _ in nodes]
    taken = [[] for _ in nodes]

    def push(time, what, node, *rest):
        heapq.heappush(queue, (round(time, 3), what > 0, next(count), what, node) + rest)

    def offer(node, part, source):
        here = nodes[node]
        js = tuple(visits[d][here[d]].index(source[d]) for d in dims)
        for d, way in routes(grid, parts[part][3], source, here):
            small = parts[part][0] in (META, LOGIT)
            entry = (not small, js[0], part, js, source)
            heapq.heappush(waiting[node].setdefault((d, way), []), entry)

    def own(node, kinds):
        for part, (kind, *_) in enumerate(parts):
            if kind in kinds:
                offer(node, part, nodes[node])

    def startable(node, slot):
        if slot == 0:
            return True
        if slot > groups * chunks:
            return False
        group, chunk = divmod(slot - 1, chunks)
        if chunk == 0:
            for g in range(groups):
                if g not in taken[node] and wanted.get((False, g), set()) <= seen[node]:
                    taken[node].append(g)
                    return True
            return False
        if group >= router_from and chunk >= chunks - 2:
            user = taken[node][2 * (group - router_from) + chunk - chunks + 2]
            return wanted.get((True, user), set()) <= seen[node]
        return True

    for node in range(len(nodes)):
        own(node, (TOKENS,))
        push(0.0, 1, node)
    while queue:
        time, _, _, what, node, *rest = heapq.heappop(queue)
        here = nodes[node]
        if what == 0:
            part, source = rest
            js = tuple(visits[d][here[d]].index(source[d]) for d in dims)
            heapq.heappush(ready[node], (js[0], time, part, js, source))
        if what in (0, 4):
            if asleep[node]:
                asleep[node] = False
                push(time, 1, node)
            continue
        if what == 2:
            own(node, (META,))
        if what == 3:
            own(node, (LOGIT,))
        slot = at_slot[node]
        if ready[node]:
            _, _, part, js, source = heapq.heappop(ready[node])
            seen[node].add((part, js))
            trace[node].append((slot, (part, js, None)))
            offer(node, part, source)
            if parts[part][0] == TOKENS and all((i, js) in seen[node] for i in range(whole)):
                trace[node].append((slot, (whole, js, CORE)))
            push(time + EVENT_TIME, 1, node)
            continue
        open_links = [
            (entries[0], link) for link, entries in waiting[node].items()
            if entries and free.get((node, link), 0.0) - time < LINK_DEPTH
        ]
        if open_links:
            turned = {d: -1 if 2 * here[d] >= grid[d] else 1 for d in dims}
            _, link = min(
                open_links, key=lambda one: (one[0][:4], one[1][0], -one[1][1] * turned[one[1][0]])
            )
            _, _, part, js, source = heapq.heappop(waiting[node][link])
            trace[node].append((slot, (part, js, link)))
            end = max(time, free.get((node, link), 0.0)) + sizes[part] / LINK_RATE
            free[(node, link)] = end
            there = dict(here)
            there[link[0]] += link[1]
            push(end + LINK_DELAY, 0, number[tuple(there.values())], part, source)
            push(time + SEND_TIME, 1, node)
            continue
        if startable(node, slot):
            at_slot[node] += 1
            if slot == 0:
                push(time + META_TIME, 2, node)
            else:
                group, chunk = divmod(slot - 1, chunks)
                push(time + times[group][chunk], 3 if slot == share_slot else 1, node)
            continue
        asleep[node] = True
        wake = [free[(node, link)] - LINK_DEPTH for link, entries in waiting[node].items() if entries]
        if wake:
            push(max(min(wake), time) + 0.01, 4, node)
    return nodes, trace, taken, time


def mirrored(grid, node, plan):
    flips = {d for d in grid if 2 * node[d] >= grid[d]}
    return [
        (at, (part, js, link if link in (None, CORE) else (link[0], -link[1] if link[0] in flips else link[1])))
        for at, (part, js, link) in plan
    ]


def make_slots(grid, parts, sizes, times, share_slot, router_from):
    nodes, trace, taken, _ = make_plan(grid, parts, sizes, times, share_slot, router_from)
    groups = len(times)
    flat = [mirrored(grid, node, plan) for node, plan in zip(nodes, trace)]
    kinds = [min(node["z"], grid["z"] - 1 - node["z"]) for node in nodes]
    known = sorted(set(kinds))
    firsts = [kinds.index(kind) for kind in known]
    same = all(
        sorted(map(repr, flat[i])) == sorted(map(repr, flat[firsts[known.index(kind)]]))
        and taken[i] == taken[firsts[known.index(kind)]]
        for i, kind in enumerate(kinds)
    )
    if same and max(grid["x"], grid["y"]) <= 2:
        table = [known.index(min(z, grid["z"] - 1 - z)) for z in range(grid["z"])]
        plans = [flat[i] for i in firsts]
        orders = [taken[i] for i in firsts]
    else:
        table, orders = [0] * grid["z"], [list(range(groups))]
        arrivals = mean_arrivals(grid, parts, sizes)
        plan, come = [], {}
        for kinds_now, at in (((TOKENS,), 0), ((META,), 1), ((LOGIT,), share_slot + 1)):
            for part, (kind, *_) in enumerate(parts):
                if kind in kinds_now:
                    plan.append((at, (part, (0, 0, 0), ALL)))
        for _, (part, js) in sorted((time, key) for key, time in arrivals.items()):
            at = share_slot + 1 if parts[part][0] == LOGIT else 1
            plan += [(at, (part, js, None)), (at, (part, js, ALL))]
            if parts[part][0] == TOKENS:
                come[js] = come.get(js, 0) + 1
                if come[js] == len(parts) - 3:
                    plan.append((at, (len(parts) - 3, js, CORE)))
        plans = [plan]
    slots = []
    for plan in plans:
        found = {}
        for at, action in plan:
            found.setdefault(at, []).append(action)
        slots.append(found)
    return table, slots, orders


class Sites:
    def __init__(self, grid, parts):
        self.index, self.shared = {}, {}
        own = len(parts)
        visits = [range(grid[d]) for d in grid]
        dims = list(grid)
        for part, (kind_of, _, _, order) in enumerate(parts):
            for js in itertools.product(*visits):
                at = dict(zip(dims, js))
                last = max((i for i, d in enumerate(order) if at[d]), default=-1)
                kinds = []
                if last >= 0 and grid[order[last]] > 2:
                    kinds.append((order[last], 0))
                for d in order[last + 1:]:
                    if grid[d] == 2:
                        kinds.append((d, 0))
                    elif grid[d] > 2:
                        kinds += [(d, 1), (d, -1)]
                if kind_of == BLOCK:
                    kinds = []
                if kind_of != TOKENS:
                    kinds.append((CORE, 0))
                for kind in kinds:
                    if kind[0] == CORE or grid[kind[0]] == 2:
                        self.index[(part, js, kind)] = part
                        self.shared[part] = self.shared.get(part, 0) + 1
                    else:
                        self.index[(part, js, kind)] = own
                        own += 1
        self.total = own

    def of(self, part, js):
        return [key[2] for key in self.index if key[0] == part and key[1] == js]


def layer_kernel(copies, flight, cap, grid, parts, sites, table, slots, orders, chunks, *refs):
    (tok_ref, og_ref, rw_ref, ids_ref, zw_ref, wg_hbm, wd_hbm,
     gu_ref, dn_ref, rout_ref, tg_ref, gathered,
     wg_ref, wd_ref, xb, ob, rows_x, rows_o, prob_ref, gate_ref, up_ref, pg_ref, hid, acc_gu, acc_dn,
     logit_ref, small_ref, spot_ref, mref, lref, rgt, back, home_dx, score_ref, home_score,
     wg_sem, wd_sem, own_sem, load_sem, send_sem, recv_sem,
     sc_send, sc_recv, dx_send, dx_recv) = refs
    d = lax.axis_index("dp")
    e = lax.axis_index("expert")
    dims = list(grid)
    top, tok_count = ids_ref.shape
    routed = rw_ref.shape[1]
    hidden_units, width = wd_ref.shape
    rows_group = flight * tok_count
    tile = min(hidden_units, 512)
    wide = min(width, 512)
    gu_rows, dn_rows = gu_ref.shape[1], dn_ref.shape[1]
    core = lax.rem(e, 2)
    my = dict(z=lax.div(d, grid["x"]), x=lax.rem(d, grid["x"]), y=lax.div(e, 2))
    visits = {k: visit_order(grid[k]) for k in dims}
    coord = {
        k: [lookup([visits[k][p][j] for p in range(grid[k])], my[k]) for j in range(grid[k])]
        for k in dims
    }

    def place(at, which):
        return (at["z"] * grid["x"] + at["x"], at["y"] * 2 + which)

    def block_index(at, which):
        dp, expert = place(at, which)
        return dp * flight + expert

    me = block_index(my, core)
    my_kind = lookup(table, my["z"])
    my_flip = 2 * my["z"] >= grid["z"]

    def slice_of(part, index):
        kind, start, rows, _ = parts[part]
        if kind == META:
            return mref.at[index]
        if kind == LOGIT:
            return lref.at[pl.ds(pl.multiple_of(index * tok_count, tok_count), tok_count), :]
        if kind == BLOCK:
            return gathered.at[index]
        return gathered.at[index, :, pl.ds(start, rows), :]

    def arrival(part, index):
        there = slice_of(part, index)
        return pltpu.make_async_remote_copy(
            src_ref=there, dst_ref=there, send_sem=send_sem.at[0],
            recv_sem=recv_sem.at[part, index], device_id=(d, e), device_id_type=MESH,
        )

    def outgoing(part, js, kind):
        at = {k: coord[k][j] for k, j in zip(dims, js)}
        dim, way = kind
        target, guard, which = dict(my), None, core
        if dim == CORE:
            which = 1 - core
        elif way == 0 and not at[dim] is my[dim] and js[dims.index(dim)]:
            ahead = my[dim] + jnp.where(at[dim] < my[dim], 1, -1)
            guard = (ahead >= 0) & (ahead < grid[dim])
            target[dim] = ahead
        elif way == 0:
            target[dim] = 1 - my[dim]
        else:
            ahead = my[dim] + way
            guard = (ahead < grid[dim]) if way > 0 else (ahead >= 0)
            target[dim] = ahead
        index = block_index(at, core)
        site = sites.index[(part, js, kind)]
        copy = pltpu.make_async_remote_copy(
            src_ref=slice_of(part, index), dst_ref=slice_of(part, index),
            send_sem=send_sem.at[site], recv_sem=recv_sem.at[part, index],
            device_id=place(target, which), device_id_type=MESH,
        )
        return guard, copy

    def launch(part, js, wanted):
        for kind in sites.of(part, js):
            if not wanted(kind):
                continue
            guard, copy = outgoing(part, js, kind)
            if guard is None:
                copy.start()
            else:
                pl.when(guard)(copy.start)

    def handle(action, flipped):
        part, js, link = action
        if link is None:
            at = {k: coord[k][j] for k, j in zip(dims, js)}
            arrival(part, block_index(at, core)).wait_recv()
            launch(part, js, lambda kind: kind[0] == CORE)
        elif link == CORE:
            launch(part, js, lambda kind: True)
        elif link == ALL:
            launch(part, js, lambda kind: kind[0] != CORE)
        elif grid[link[0]] > 2 and not js[dims.index(link[0])]:
            pl.when(flipped)(lambda: launch(part, js, lambda kind: kind == (link[0], -link[1])))
            pl.when(~flipped)(lambda: launch(part, js, lambda kind: kind == link))
        else:
            launch(part, js, lambda kind: kind[0] == link[0])

    def run_actions(slot):
        for kind, found in enumerate(slots):
            if slot in found:
                @pl.when(my_kind == kind)
                def _():
                    for action in found[slot]:
                        handle(action, my_flip)

    def run_steps(j, chunk):
        def tree(found, ks):
            ks = [k for k in ks if 1 + k * chunks + chunk in found]
            if len(ks) == 1:
                @pl.when(j == ks[0])
                def _():
                    for action in found[1 + ks[0] * chunks + chunk]:
                        handle(action, my_flip)
            elif ks:
                cut = ks[len(ks) // 2]
                pl.when(j < cut)(lambda: tree(found, [k for k in ks if k < cut]))
                pl.when(j >= cut)(lambda: tree(found, [k for k in ks if k >= cut]))

        for kind, found in enumerate(slots):
            if any(1 + k * chunks + chunk in found for k in range(copies)):
                pl.when(my_kind == kind)(lambda: tree(found, list(range(copies))))

    home = (0,) * len(dims)

    def start_own(kinds):
        for part, (kind, *_) in enumerate(parts):
            if kind in kinds:
                launch(part, home, lambda kind: kind[0] == CORE)

    barrier = pltpu.get_barrier_semaphore()
    for k in range(1, flight):
        pl.semaphore_signal(
            barrier, inc=1, device_id=(d, lax.rem(e + k, flight)), device_id_type=MESH
        )
    greeted = jnp.int32(flight - 1)
    for k in ("z", "x"):
        for way in (1, -1):
            ahead = my[k] + way
            there = (ahead < grid[k]) if way > 0 else (ahead >= 0)
            greeted = greeted + jnp.where(there, 1, 0)

            @pl.when(there)
            def _():
                target = dict(my)
                target[k] = ahead
                pl.semaphore_signal(
                    barrier, inc=1, device_id=place(target, core), device_id_type=MESH
                )

    load_g = pltpu.make_async_copy(wg_hbm, wg_ref, wg_sem)
    load_d = pltpu.make_async_copy(wd_hbm, wd_ref, wd_sem)
    load_g.start()
    load_d.start()
    mine = pl.ds(pl.multiple_of(me * tok_count, tok_count), tok_count)
    own_x = pltpu.make_async_copy(tok_ref, gathered.at[me, 0], own_sem.at[0])
    own_o = pltpu.make_async_copy(og_ref, gathered.at[me, 1], own_sem.at[1])
    own_x.start()
    own_o.start()
    own_x.wait()
    own_o.wait()
    pl.semaphore_wait(barrier, greeted)
    run_actions(0)
    start_own((BLOCK,))

    lanes = lax.broadcasted_iota(jnp.int32, (tok_count, routed), 1)

    def column(row):
        return jnp.broadcast_to(row, (routed, tok_count)).T

    ids = [column(ids_ref[k:k + 1, :].astype(F32)).astype(jnp.int32) for k in range(top)]
    choose = [column_ids == lanes for column_ids in ids]
    member = sum(c.astype(F32) for c in choose)
    earlier = lax.broadcasted_iota(jnp.int32, (tok_count, tok_count), 0) > (
        lax.broadcasted_iota(jnp.int32, (tok_count, tok_count), 1)
    )
    rank = jnp.dot(earlier.astype(F32).astype(BF16), member.astype(BF16), preferred_element_type=F32)
    rank = jnp.where(member > 0.0, rank, -1.0)
    logits = jnp.dot(tok_ref[...], rw_ref[...], preferred_element_type=F32)
    chosen = [
        jnp.exp(jnp.sum(jnp.where(c, logits, 0.0), axis=1, keepdims=True)) for c in choose
    ]
    norm = sum(chosen)
    probs = [c / norm for c in chosen]
    weight = jnp.zeros(lanes.shape, F32)
    for k in range(top):
        weight = weight + jnp.where(choose[k], probs[k], 0.0)
    mref[me, 0:flight, :] = rank.T[0:flight, :]
    mref[me, flight:2 * flight, :] = weight.T[0:flight, :]
    start_own((META,))
    logit_ref[...] = logits
    log_total = jnp.log(jnp.sum(jnp.exp(logits), axis=1, keepdims=True))
    small = jnp.where(lanes == top, log_total, column(zw_ref[...]))
    spot = jnp.full(lanes.shape, -1, jnp.int32)
    spots = jnp.where((rank >= 0.0) & (lanes < flight), rank + (lanes * cap).astype(F32) + 1.0, 0.0)
    for k in range(top):
        small = jnp.where(lanes == k, probs[k], small)
        at = jnp.sum(jnp.where(choose[k], spots, 0.0), axis=1, keepdims=True) - 1.0
        spot = jnp.where(lanes == k, at.astype(jnp.int32), spot)
        spot = jnp.where(lanes == top + k, ids[k], spot)
    small_ref[...] = small
    spot_ref[...] = spot
    acc_gu[...] = jnp.zeros_like(acc_gu)
    acc_dn[...] = jnp.zeros_like(acc_dn)
    rgt[...] = jnp.zeros_like(rgt)

    window = acc_dn.shape[0]
    dn_unit = math.gcd(dn_rows, 128)
    dn_start = jnp.minimum(lax.div(d * dn_rows, 128) * 128, hidden_units - window)
    dn_off = pl.multiple_of(d * dn_rows - dn_start, dn_unit)
    dn_start = pl.multiple_of(dn_start, 128)

    def group_at(j):
        g = lookup(sum(orders, []), my_kind * copies + j)
        jz, jx = lax.div(g, grid["x"]), lax.rem(g, grid["x"])
        z = lookup(sum(visits["z"], []), my["z"] * grid["z"] + jz)
        x = lookup(sum(visits["x"], []), my["x"] * grid["x"] + jx)
        return z * grid["x"] + x

    def wait_sibling(group, kinds):
        for y in range(grid["y"]):
            index = group * flight + 2 * y + 1 - core
            for part, (kind, *_) in enumerate(parts):
                if kind in kinds:
                    arrival(part, index).wait_recv()

    def reload_x(group):
        blocks = pl.ds(pl.multiple_of(group * flight, flight), flight)
        return pltpu.make_async_copy(gathered.at[blocks, 0], ob, load_sem.at[1])

    def load_x(group):
        blocks = pl.ds(pl.multiple_of(group * flight, flight), flight)
        return pltpu.make_async_copy(gathered.at[blocks, 0], xb, load_sem.at[0])

    def load_o(group):
        blocks = pl.ds(pl.multiple_of(group * flight, flight), flight)
        return pltpu.make_async_copy(gathered.at[blocks, 1], ob, load_sem.at[1])

    ranks = lax.broadcasted_iota(jnp.int32, (2 * cap, 2 * tok_count), 0).astype(F32)

    def pair_rank(group, pair):
        index = group * flight + 2 * pair
        first = mref[index, pl.ds(e, 1), :]
        second = mref[index + 1, pl.ds(e, 1), :]
        second = jnp.where(second >= 0.0, second + float(cap), -1.0)
        return jnp.concatenate([first, second], axis=1) == ranks

    def pick_rows(group, source, target):
        for pair in range(flight // 2):
            picks = pair_rank(group, pair).astype(F32).astype(BF16)
            target[pair * 2 * cap:(pair + 1) * 2 * cap, :] = jnp.dot(
                picks, source[2 * pair:2 * pair + 2].reshape(2 * tok_count, width),
                preferred_element_type=F32,
            ).astype(BF16)

    def gather_x(group):
        wait_sibling(group, (BLOCK, META))
        load_x(group).start()
        load_o(group).start()
        for pair in range(flight // 2):
            index = group * flight + 2 * pair
            weights = jnp.concatenate(
                [mref[index + i, pl.ds(flight + e, 1), :] for i in range(2)], axis=1
            )
            part = jnp.where(pair_rank(group, pair), weights, 0.0)
            prob = jnp.sum(part, axis=1, keepdims=True)
            prob_ref[pair * 2 * cap:(pair + 1) * 2 * cap, :] = jnp.broadcast_to(
                prob, (2 * cap, prob_ref.shape[1])
            )
        load_x(group).wait()
        pick_rows(group, xb, rows_x)

    def gather_o(group):
        load_o(group).wait()
        pick_rows(group, ob, rows_o)

    def gate_tile(col):
        gate_ref[...] = jnp.dot(
            rows_x[...], wg_ref[:, col:col + tile], preferred_element_type=F32
        )

    def up_tile(col):
        up_ref[...] = jnp.dot(
            rows_x[...], wg_ref[:, hidden_units + col:hidden_units + col + tile],
            preferred_element_type=F32,
        )

    def hidden_tile(col, own):
        gate, up = gate_ref[...], up_ref[...]
        raw = lax.dot_general(
            rows_o[...], wd_ref[col:col + tile, :], (((1,), (1,)), ((), ())),
            preferred_element_type=F32,
        )
        sig = jax.nn.sigmoid(gate)
        active = gate * sig
        hidden = (active * up).astype(BF16)
        hid[:, col:col + tile] = hidden
        grad = prob_ref[:, 0:1] * raw
        pg_ref[:, col:col + tile] = (grad * up * sig * (1.0 + gate * (1.0 - sig))).astype(BF16)
        pg_ref[:, hidden_units + col:hidden_units + col + tile] = (grad * active).astype(BF16)

        @pl.when(own)
        def _():
            part = jnp.sum(raw * hidden.astype(F32), axis=1, keepdims=True)
            part = jnp.broadcast_to(part, score_ref.shape)
            score_ref[...] = part if col == 0 else score_ref[...] + part

    def up_grads():
        rows_o[...] = (prob_ref[:, 0:1] * rows_o[...].astype(F32)).astype(BF16)
        taken = rows_x[:, pl.ds(pl.multiple_of(d * gu_rows, gu_rows), gu_rows)]
        for col in range(0, 2 * hidden_units, tile):
            acc_gu[:, col:col + tile] += lax.dot_general(
                taken, pg_ref[:, col:col + tile], (((0,), (0,)), ((), ())),
                preferred_element_type=F32,
            )

    def down_grads():
        taken = hid[:, pl.ds(dn_start, window)]
        for col in range(0, width, wide):
            acc_dn[:, col:col + wide] += lax.dot_general(
                taken, rows_o[:, col:col + wide], (((0,), (0,)), ((), ())),
                preferred_element_type=F32,
            )

    def block(ref, index):
        return ref.at[pl.ds(pl.multiple_of(index * cap, cap), cap), :]

    def give_score(k, source):
        to = lax.rem(e + k, flight)
        return pltpu.make_async_remote_copy(
            src_ref=block(score_ref, to), dst_ref=home_score.at[source],
            send_sem=sc_send.at[k - 1], recv_sem=sc_recv.at[k - 1],
            device_id=(d, to), device_id_type=MESH,
        )

    def give_dx(k, source):
        to = lax.rem(e + k, flight)
        return pltpu.make_async_remote_copy(
            src_ref=block(back, to), dst_ref=block(home_dx, source),
            send_sem=dx_send.at[k - 1], recv_sem=dx_recv.at[k - 1],
            device_id=(d, to), device_id_type=MESH,
        )

    def from_peer(k):
        return lax.rem(e + flight - k, flight)

    def one_hot(k):
        across = lax.broadcasted_iota(jnp.int32, (tok_count, flight * cap), 1)
        return across == spot_ref[:, k:k + 1]

    def row_grads(first, last):
        for col in range(first, last, wide):
            back[:, col:col + wide] = lax.dot_general(
                pg_ref[...], wg_ref[col:col + wide, :], (((1,), (1,)), ((), ())),
                preferred_element_type=F32,
            ).astype(BF16)

    half = width // 2 // wide * wide

    def send_scores():
        for k in range(1, flight):
            give_score(k, e).start()
        home_score[e] = score_ref[pl.ds(pl.multiple_of(e * cap, cap), cap), :]
        row_grads(0, half)

    def send_rows():
        row_grads(half, width)
        for k in range(1, flight):
            give_dx(k, e).start()
        own_rows = pl.ds(pl.multiple_of(e * cap, cap), cap)
        home_dx[own_rows, :] = back[own_rows, :]

    def logit_grads():
        for k in range(1, flight):
            give_score(k, from_peer(k)).wait_recv()
        arrived = home_score[...].reshape(flight * cap, home_score.shape[2])
        logits = logit_ref[...]
        scores = [
            jnp.dot(
                one_hot(k).astype(F32), arrived,
                precision=lax.Precision.HIGHEST, preferred_element_type=F32,
            )
            for k in range(top)
        ]
        probs = [small_ref[:, k:k + 1] for k in range(top)]
        mean = sum(p * q for p, q in zip(probs, scores))
        z_weight = small_ref[:, top + 1:top + 2]
        log_total = small_ref[:, top:top + 1]
        grad = 2.0 * z_weight * log_total * jnp.exp(logits - log_total)
        for k in range(top):
            grad = grad + jnp.where(
                spot_ref[:, top + k:top + k + 1] == lanes, probs[k] * (scores[k] - mean), 0.0
            )
        lref[mine, :] = grad.astype(BF16)
        start_own((LOGIT,))

    def token_grads():
        for k in range(1, flight):
            give_dx(k, from_peer(k)).wait_recv()
        picks = sum(one_hot(k).astype(F32) for k in range(top)).astype(BF16)
        own_lg = lref[mine, :]
        for col in range(0, width, wide):
            total = jnp.dot(picks, home_dx[:, col:col + wide], preferred_element_type=F32)
            total = total + lax.dot_general(
                own_lg, rw_ref[col:col + wide, :], (((1,), (1,)), ((), ())),
                preferred_element_type=F32,
            )
            tg_ref[:, col:col + wide] = total.astype(BF16)

    def router(group, held):
        wait_sibling(group, (LOGIT,))
        rows = pl.ds(pl.multiple_of(group * rows_group, rows_group), rows_group)
        grad = lref[rows, :].astype(F32).T.astype(BF16)
        for col in range(0, width, wide):
            rgt[:, col:col + wide] += jnp.dot(
                grad, held[:, :, col:col + wide].reshape(rows_group, wide), preferred_element_type=F32
            )

    tiles = hidden_units // tile

    def step(j, carry):
        group = group_at(j)
        own = j == 0
        late_half = j >= copies // 2
        early = group_at(jnp.maximum(2 * (j - copies // 2), 0))
        second = group_at(jnp.maximum(2 * (j - copies // 2) + 1, 0))

        spot_now = [0]

        def then(run):
            chunk = spot_now[0]
            spot_now[0] += 1
            run_steps(j, chunk)
            run()

        def first_rows():
            gather_x(group)

            @pl.when(late_half & (j < copies - 1))
            def _():
                load_x(second).start()

            @pl.when(own)
            def _():
                load_g.wait()
                load_d.wait()

        def second_rows():
            gather_o(group)

            @pl.when(late_half)
            def _():
                reload_x(early).start()

        then(first_rows)
        then(second_rows)
        for index in range(tiles):
            then(functools.partial(gate_tile, index * tile))
            then(functools.partial(up_tile, index * tile))
            then(functools.partial(hidden_tile, index * tile, own))
        then(up_grads)
        then(down_grads)

        def special():
            pl.when(j == 0)(send_scores)
            pl.when(j == 1)(logit_grads)
            pl.when(j == 2)(token_grads)

            @pl.when(late_half)
            def _():
                reload_x(early).wait()
                router(early, ob)

        def special_late():
            pl.when(j == 0)(send_rows)

            @pl.when(late_half)
            def _():
                @pl.when(j < copies - 1)
                def _():
                    load_x(second).wait()

                router(second, xb)

        then(special)
        then(special_late)
        return carry

    lax.fori_loop(0, copies, step, 0)
    run_actions(1 + copies * chunks)
    gu_ref[0] = acc_gu[...].astype(BF16)
    dn_ref[0] = acc_dn[pl.ds(dn_off, dn_rows), :].astype(BF16)
    rout_ref[...] = rgt[...].T
    for part, count in sites.shared.items():
        kind, start, rows, _ = parts[part]
        if kind == META:
            sent = mref.at[pl.ds(0, count)]
        elif kind == LOGIT:
            sent = lref.at[pl.ds(0, count * tok_count), :]
        elif kind == BLOCK:
            sent = gathered.at[pl.ds(0, count)]
        else:
            sent = gathered.at[pl.ds(0, count), :, pl.ds(start, rows), :]
        pltpu.make_async_remote_copy(
            src_ref=sent, dst_ref=sent, send_sem=send_sem.at[part], recv_sem=recv_sem.at[part, 0],
            device_id=(d, lax.rem(e + 1, flight)), device_id_type=MESH,
        ).wait_send()
    for (part, js, kind), site in sites.index.items():
        if site >= len(parts):
            guard, copy = outgoing(part, js, kind)
            pl.when(guard)(copy.wait_send)
    for k in range(1, flight):
        give_score(k, e).wait_send()
        give_dx(k, e).wait_send()


def finish_kernel(*refs):
    sources, targets, holds, sems = refs[:4], refs[4:8], refs[8:12], refs[12]
    takes = [
        pltpu.make_async_copy(source, hold, sems.at[i])
        for i, (source, hold) in enumerate(zip(sources, holds))
    ]
    gives = [
        pltpu.make_async_copy(hold, target, sems.at[4 + i])
        for i, (hold, target) in enumerate(zip(holds, targets))
    ]
    for take in takes:
        take.start()
    for take, give in zip(takes, gives):
        take.wait()
        give.start()
    for give in gives:
        give.wait()


def per_device(tokens, out_grad, z_weight, router_weight, expert_ids, gate_up_weight, down_weight):
    n = lax.axis_size("dp")
    flight = lax.axis_size("expert")
    w_gateup, w_down = gate_up_weight[0], down_weight[0]
    tok_count, width = tokens.shape
    routed = router_weight.shape[1]
    hidden = w_down.shape[0]
    gate_up = w_gateup.shape[1]
    cap = tok_count // 2
    rows = flight * cap
    gu_rows, dn_rows = width // n, hidden // n
    window = min(hidden, (dn_rows + 127) // 128 * 128 + 128)
    if dn_rows % 128 == 0:
        window = dn_rows
    elif dn_rows + (128 - math.gcd(dn_rows, 128)) <= window - 128:
        window -= 128
    grid = grid_of(n, flight)
    parts = make_parts(grid, tok_count)
    sites = Sites(grid, parts)
    sizes = [p[2] * width * 4 for p in parts]
    sizes[-2], sizes[-1] = 8 * flight * tok_count, 2 * tok_count * routed
    tiles = hidden // min(hidden, 512)
    base = [1.9, 1.0] + [0.57, 0.57, 0.75] * tiles + [0.75, 0.55]
    chunk_times = [
        base + ([2.0, 2.0] if j == 0 else [1.6, 0.1] if j < 3 else [0.1, 0.1] if j < n // 2 else [0.8, 0.8])
        for j in range(n)
    ]
    chunks = len(base) + 2
    share_slot = 1 + chunks + len(base)
    table, slots, orders = make_slots(grid, parts, sizes, chunk_times, share_slot, n // 2)
    dma = pltpu.SemaphoreType.DMA
    vmem = pl.BlockSpec(memory_space=pltpu.VMEM)
    hbm = pl.BlockSpec(memory_space=pl.ANY)
    shape = jax.ShapeDtypeStruct
    blocks = n * flight
    gate_up_grad, down_grad, router_grad, token_grad, _ = pl.pallas_call(
        functools.partial(
            layer_kernel, n, flight, cap, grid, parts, sites, table, slots, orders, chunks
        ),
        out_shape=(
            shape((1, gu_rows, gate_up), BF16),
            shape((1, dn_rows, width), BF16),
            shape((width, routed), F32),
            shape((tok_count, width), BF16),
            shape((blocks, 2, tok_count, width), BF16),
        ),
        in_specs=[vmem] * 5 + [hbm] * 2,
        out_specs=(vmem,) * 4 + (hbm,),
        scratch_shapes=[
            pltpu.VMEM(w_gateup.shape, BF16),
            pltpu.VMEM(w_down.shape, BF16),
            pltpu.VMEM((flight, tok_count, width), BF16),
            pltpu.VMEM((flight, tok_count, width), BF16),
            pltpu.VMEM((rows, width), BF16),
            pltpu.VMEM((rows, width), BF16),
            pltpu.VMEM((rows, 128), F32),
            pltpu.VMEM((rows, min(hidden, 512)), F32),
            pltpu.VMEM((rows, min(hidden, 512)), F32),
            pltpu.VMEM((rows, gate_up), BF16),
            pltpu.VMEM((rows, hidden), BF16),
            pltpu.VMEM((gu_rows, gate_up), F32),
            pltpu.VMEM((window, width), F32),
            pltpu.VMEM((tok_count, routed), F32),
            pltpu.VMEM((tok_count, routed), F32),
            pltpu.VMEM((tok_count, routed), jnp.int32),
            pltpu.VMEM((blocks, 2 * flight, tok_count), F32),
            pltpu.VMEM((blocks * tok_count, routed), BF16),
            pltpu.VMEM((routed, width), F32),
            pltpu.VMEM((rows, width), BF16),
            pltpu.VMEM((rows, width), BF16),
            pltpu.VMEM((rows, routed), F32),
            pltpu.VMEM((flight, cap, routed), F32),
            dma, dma, dma((2,)), dma((2,)),
            dma((sites.total,)), dma((len(parts), blocks)),
        ] + [dma((flight - 1,))] * 4,
        compiler_params=pltpu.CompilerParams(
            collective_id=0, has_side_effects=True, vmem_limit_bytes=67_000_000
        ),
        name="layer",
    )(
        tokens,
        out_grad,
        router_weight,
        expert_ids.T,
        z_weight[None, :],
        w_gateup,
        w_down,
    )
    results = (token_grad, router_grad, gate_up_grad, down_grad)
    return pl.pallas_call(
        finish_kernel,
        out_shape=tuple(shape(r.shape, r.dtype) for r in results),
        in_specs=[hbm] * 4,
        out_specs=(hbm,) * 4,
        scratch_shapes=[pltpu.VMEM(r.shape, r.dtype) for r in results] + [dma((8,))],
        compiler_params=pltpu.CompilerParams(vmem_limit_bytes=67_000_000),
        name="finish",
    )(*results)


def solution(mesh):
    return jax.shard_map(
        per_device,
        mesh=mesh,
        in_specs=(
            P(("dp", "expert"), None),
            P(("dp", "expert"), None),
            P(("dp", "expert")),
            P(),
            P(("dp", "expert"), None),
            P("expert", None, None),
            P("expert", None, None),
        ),
        out_specs=(
            P(("dp", "expert"), None),
            P(),
            P("expert", "dp", None),
            P("expert", "dp", None),
        ),
        check_vma=False,
    )
```
